32 devices in a mesh: north: 8 (over z, x), deep: 4 (over y, core).
Axes of the slice: x: 2, y: 2, z: 4, core: 2. Of those that a mesh axis runs over, the one named last changes fastest.
Arguments:
- source: float32 [128, 128, 2048], P(None, 'north', 'deep'), may hold values from -6 to 6
- symbol_x: float32 [128], replicated, may hold values from 0.3 to 3
- symbol_y: float32 [128], replicated, may hold values from 0.3 to 3
- symbol_z: float32 [2048], replicated, may hold values from 0.3 to 3
Outputs:
- coefficients: float32 [64, 64, 1024], P('north', 'deep')
The draws below stay inside these ranges and needn't reach their ends.
All inputs are finite; a program needn't handle non-finite values.
Results may differ from the reference program's by a relative error of at most 0.000071.
Values sent between devices are 32-bit elements; how exact they have to be, the bound alone decides.
A program may use at most 128 MiB of HBM per device.

```python
import jax
import jax.numpy as jnp
from jax import lax

GRID_X = 128
GRID_Y = 128
GRID_Z = 2048


def block_levels(stream_key, shape, shards, least, largest):
    gain = 1.0
    for dim, parts in shards:
        heights = jax.random.uniform(jax.random.fold_in(jax.random.fold_in(stream_key, 6), dim), (parts,), jnp.float32, least / len(shards), largest / len(shards))
        gain = gain * jnp.repeat(jnp.exp(heights), shape[dim] // parts).reshape((-1,) + (1,) * (len(shape) - 1 - dim))
    return gain


def noise(rng, shape, scale, most, shards=(), dtype=jnp.bfloat16):
    level = block_levels(rng, shape, shards, -0.22, 0.18) if shards else 1.0
    entries = jax.random.normal(rng, shape, jnp.float32) * scale * level
    return jnp.minimum(jnp.maximum(entries, -most), most).astype(dtype)


def setup_inputs(seed: int = 0) -> dict:
    arg_keys = jax.random.split(jax.random.key(seed), 5)
    source = noise(arg_keys[0], (GRID_X, GRID_Y, GRID_Z), 1.0, 6.0, ((1, 8), (2, 4)), jnp.float32)
    symbol_x = jnp.clip(jax.random.uniform(arg_keys[1], (GRID_X,), jnp.float32, 0.3, 3.0), 0.3, 3.0)
    symbol_y = jnp.clip(jax.random.uniform(arg_keys[2], (GRID_Y,), jnp.float32, 0.3, 3.0), 0.3, 3.0)
    symbol_z = jnp.clip(jax.random.uniform(arg_keys[3], (GRID_Z,), jnp.float32, 0.3, 3.0), 0.3, 3.0)
    return {"source": source, "symbol_x": symbol_x, "symbol_y": symbol_y, "symbol_z": symbol_z}


def basis_table(count):
    rank = jnp.arange(count)
    angle = jnp.pi / (count + 1) * ((rank[:, None] + 1) * (rank[None, :] + 1) % (2 * count + 2)).astype(jnp.float32)
    return jnp.sin(angle) * (2.0 / (count + 1)) ** 0.5

def along_dim(values, dim):
    moved = jnp.tensordot(values, basis_table(values.shape[dim]), axes=([dim], [0]), precision=lax.Precision.HIGHEST)
    return jnp.moveaxis(moved, -1, dim)

def reference(source, symbol_x, symbol_y, symbol_z):
    coefficients = source
    coefficients = along_dim(coefficients, 0)
    coefficients = lax.slice_in_dim(coefficients, 0, GRID_X // 2, axis=0)
    coefficients = along_dim(coefficients, 1)
    coefficients = lax.slice_in_dim(coefficients, 0, GRID_Y // 2, axis=1)
    coefficients = along_dim(coefficients, 2)
    coefficients = lax.slice_in_dim(coefficients, 0, GRID_Z // 2, axis=2)
    symbol = symbol_x[:GRID_X // 2][:, None, None] + symbol_y[:GRID_Y // 2][None, :, None] + symbol_z[:GRID_Z // 2][None, None, :]
    coefficients = coefficients * lax.rsqrt(symbol)
    return coefficients
```

```python
import functools

import jax
import jax.numpy as jnp
import numpy as np
from jax import lax
from jax.experimental import pallas as pl
from jax.experimental.pallas import tpu as pltpu
from jax.sharding import PartitionSpec as P

F32, BF16 = jnp.float32, jnp.bfloat16
FINE = 32
TILE = 256
SUB = 8
ROWS = 64


def angles(rows, modes, count):
    rank = np.outer(rows, modes) % (2 * count + 2)
    return np.pi / (count + 1) * rank


def split_np(table):
    high = table.astype(np.float32).astype(BF16)
    low = (table - high.astype(np.float64)).astype(np.float32).astype(BF16)
    return high, low


def left_table(count):
    gain = (2.0 / (count + 1)) ** 0.5
    table = np.sin(angles(np.arange(1, count // 2 + 1), np.arange(1, count + 1), count)) * gain
    return split_np(table)


def stacked(high, low):
    return np.block([[high, high], [low, np.zeros_like(low)]])


def long_tables(count):
    modes = np.arange(1, count // 2 + 1)
    gain = (2.0 / (count + 1)) ** 0.5
    coarse = angles(np.arange(0, count, FINE), modes, count)
    step = angles(np.arange(1, FINE + 1), modes, count)
    f32 = lambda v: jnp.asarray(v.astype(np.float32))
    return f32(np.sin(coarse) * gain), f32(np.cos(coarse) * gain), f32(np.sin(step)), f32(np.cos(step))


def split(values):
    high = values.astype(BF16)
    return high, (values - high.astype(F32)).astype(BF16)


def dot(a, b):
    return jnp.dot(a, b, preferred_element_type=F32)


def loop(count, body):
    if count == 1:
        body(0)
    else:
        lax.fori_loop(0, count, lambda i, c: (body(i), c)[1], 0)


def kernel(
    north, deep, each,
    src, tx, ty, sin_a, cos_a, sin_b, cos_b, symbol_x, symbol_y, symbol_z,
    out,
    field, turned, send1, recv1, send2, recv2, send3, recv3, t_high, t_low, left_all, left,
    fs, s1, r1, s2, r2, s3, r3,
):
    me_n, me_d = lax.axis_index("north"), lax.axis_index("deep")
    nx, ny_part, nz_part = src.shape
    halves = ny_part // SUB
    kept_z = t_high.shape[1]
    kept_y = ny_part * north // 2
    share_y = kept_y // deep
    half = north // 2
    pairs = deep // 2
    my_pair = me_d // 2
    far = jnp.where(me_n < half, half, 0)
    bases = (far, half - far)
    last = each - 1

    pieces = [(h, c) for h in range(halves) for c in range(0, nz_part, TILE)]
    loads = {}
    for i, (h, c) in enumerate(pieces):
        loads[h, c] = pltpu.make_async_copy(
            src.at[:, h * SUB : (h + 1) * SUB, c : c + TILE], field.at[h, :, :, c : c + TILE], fs.at[i]
        )
        loads[h, c].start()

    barrier = pltpu.get_barrier_semaphore()
    for r in range(1, deep):
        pl.semaphore_signal(barrier, inc=1, device_id={"deep": lax.rem(me_d + r, deep)})
    for r in range(1, north):
        pl.semaphore_signal(barrier, inc=1, device_id={"north": lax.rem(me_n + r, north)})

    def x_product(h, c):
        loads[h, c].wait()
        block = min(nx, 128)

        def turn(g):
            for k in range(0, block, 16):
                at = pl.multiple_of(g * block + k, 16)
                high, low = split(jnp.swapaxes(field[h, pl.ds(at, 16), :, c : c + TILE], 0, 1))
                turned[:, pl.ds(at, 16), :] = high
                turned[:, pl.ds(pl.multiple_of(nx + at, 16), 16), :] = low

        loop(nx // block, turn)
        rows = tx.shape[1] // 2
        group = rows // north

        def modes_of(g):
            modes = []
            for y in range(SUB):
                both = dot(tx[g], turned[y])
                modes.append(both[:rows] + both[rows:])
            for k in range(group):
                block = jnp.stack([m[k * north : (k + 1) * north] for m in modes])
                ed = g * group + k
                send1[ed // deep, lax.rem(ed, deep), h, :, :, c : c + TILE] = jnp.swapaxes(block, 0, 1)

        loop(tx.shape[0], modes_of)

    copies1 = {}

    def send_modes(f, e, h):
        for r in (*range(2, deep), 1):
            to = lax.bitwise_xor(me_d, r)
            at = pl.ds(bases[f], half)
            slot = (f * each + e) * halves + h
            copies1[f, e, h, r] = pltpu.make_async_remote_copy(
                src_ref=send1.at[e, to, h, at],
                dst_ref=recv1.at[e, me_d, h, at],
                send_sem=s1.at[slot, r],
                recv_sem=r1.at[slot, r],
                device_id={"deep": to},
            )
            copies1[f, e, h, r].start()

    chunks = [(f, e, h) for f in range(2) for e in range(each) for h in range(halves)]
    for h in range(halves):
        for c in range(0, nz_part, TILE):
            x_product(h, c)
        if h == 0:
            pl.semaphore_wait(barrier, deep + north - 2)
            send_modes(*chunks[0])
    for chunk in chunks[1:]:
        send_modes(*chunk)

    def table_step(a):
        table = sin_a[pl.ds(a, 1), :] * cos_b[...] + cos_a[pl.ds(a, 1), :] * sin_b[...]
        high, low = split(table)
        at = pl.multiple_of(a * FINE, FINE)
        t_high[pl.ds(at, FINE), :] = high
        t_low[pl.ds(at, FINE), :] = low

    loop(sin_a.shape[0], table_step)

    rows = half * SUB

    def z_product(lhs, count, pair):
        at = pl.multiple_of(pair * 2 * nz_part, 2 * nz_part)
        for c in range(0, kept_z, TILE):
            both = dot(lhs[...], t_high[pl.ds(at, 2 * nz_part), c : c + TILE])
            yield c, both[:count] + both[count:] + dot(
                lhs[:count, :], t_low[pl.ds(at, 2 * nz_part), c : c + TILE]
            )

    for chunk in chunks:
        copies1[(*chunk, 1)].wait_recv()
    total = rows * 2

    def near_part(k):
        e, h = k // halves, lax.rem(k, halves)
        for owner, block in ((me_d, send1), (lax.bitwise_xor(me_d, 1), recv1)):
            high, low = split(block[e, owner, h].reshape(total, nz_part))
            cols = pl.ds(pl.multiple_of(lax.rem(owner, 2) * nz_part, nz_part), nz_part)
            left_all[:total, cols] = high
            left_all[total:, cols] = low
        for c, value in z_product(left_all, total, my_pair):
            send2[e, h, :, :, c : c + TILE] = value.reshape(north, SUB, TILE)

    loop(each * halves, near_part)

    def inverse_roots():
        row = lax.broadcasted_iota(jnp.int32, (share_y, TILE), 0)
        part_y = jnp.zeros((share_y, TILE), F32)
        for j in range(share_y):
            part_y = jnp.where(row == j, symbol_y[me_d * share_y + j], part_y)
        for d in range(deep):
            for e in range(each):
                part_x = symbol_x[me_n * deep * each + d * each + e]
                for c in range(0, kept_z, TILE):
                    out[d, e, :, c : c + TILE] = lax.rsqrt(part_x + part_y + symbol_z[:, c : c + TILE])

    inverse_roots()

    def copy2(e, h, n):
        return pltpu.make_async_remote_copy(
            src_ref=send2.at[e, h, n],
            dst_ref=recv2.at[e, h, me_n],
            send_sem=s2.at[e * halves + h, n],
            recv_sem=r2.at[e * halves + h, me_n],
            device_id={"north": n},
        )

    def arrival2(e, h, n):
        return pltpu.make_async_remote_copy(
            src_ref=send2.at[e, h, n],
            dst_ref=recv2.at[e, h, n],
            send_sem=s2.at[e * halves + h, n],
            recv_sem=r2.at[e * halves + h, n],
            device_id={"north": n},
        )

    def others():
        for r in range(north - 1):
            yield r + (r >= me_n).astype(jnp.int32)

    copies3 = {}

    def y_stage(e, parts):
        for h in range(halves):
            for n in others():
                arrival2(e, h, n).wait_recv()
        width = kept_z // parts
        for p in range(parts):
            for c in range(p * width, (p + 1) * width, TILE):
                values = recv2[e, :, :, :, c : c + TILE].reshape(ny_part * north, TILE)
                both = dot(ty[...], jnp.concatenate(split(values), axis=0))
                modes = both[:kept_y] + both[kept_y:]
                send3[e, :, :, c : c + TILE] = modes.reshape(deep, share_y, TILE)
            cols = pl.ds(p * width, width)
            for r in (*range(2, deep), 1):
                to = lax.bitwise_xor(me_d, r)
                copies3[e, p, r] = pltpu.make_async_remote_copy(
                    src_ref=send3.at[e, to, :, cols],
                    dst_ref=recv3.at[me_d, e, :, cols],
                    send_sem=s3.at[e * 2 + p, r],
                    recv_sem=r3.at[e * 2 + p, r],
                    device_id={"deep": to},
                )
                copies3[e, p, r].start()

    for f, e, h in chunks:
        for pair in range(1, pairs):
            other = lax.rem(my_pair + pair, pairs)
            for k in range(2):
                owner = other * 2 + k
                r = lax.bitwise_xor(owner, me_d)
                slot = (f * each + e) * halves + h
                at = pl.ds(bases[f], half)
                pltpu.make_async_remote_copy(
                    src_ref=send1.at[e, owner, h, at],
                    dst_ref=recv1.at[e, owner, h, at],
                    send_sem=s1.at[slot, r],
                    recv_sem=r1.at[slot, r],
                    device_id={"deep": owner},
                ).wait_recv()
                high, low = split(recv1[e, owner, h, at].reshape(rows, nz_part))
                left[:rows, k * nz_part : (k + 1) * nz_part] = high
                left[rows:, k * nz_part : (k + 1) * nz_part] = low
            for c, value in z_product(left, rows, other):
                send2[e, h, at, :, c : c + TILE] += value.reshape(half, SUB, TILE)
        for i in range(half):
            n = bases[f] + i
            if f == 0:
                copy2(e, h, n).start()
            else:
                pl.when(n != me_n)(lambda: copy2(e, h, n).start())
        if f == 1:
            recv2[e, h, me_n] = send2[e, h, me_n]
            if h == halves - 1 and e < last:
                y_stage(e, 1)
    y_stage(last, 2)

    for copy in copies1.values():
        copy.wait_send()
    for e in range(each):
        for h in range(halves):
            for n in others():
                arrival2(e, h, n).wait_send()
    for e in range(each):
        out[me_d, e] = out[me_d, e] * send3[e, me_d]
        for p in range(2 if e == last else 1):
            for r in (1, *range(2, deep)):
                copy = copies3[e, p, r]
                copy.wait()
                width = kept_z // 2 if e == last else kept_z
                cols = slice(p * width, (p + 1) * width)
                owner = lax.bitwise_xor(me_d, r)
                out[owner, e, :, cols] = out[owner, e, :, cols] * recv3[owner, e, :, cols]


def on_device(source, symbol_x, symbol_y, symbol_z):
    north, deep = lax.axis_size("north"), lax.axis_size("deep")
    nx, ny_part, nz_part = source.shape
    each, halves = nx // 2 // north // deep, ny_part // SUB
    ny, nz = ny_part * north, nz_part * deep
    kept_z, share_y = nz // 2, ny // 2 // deep
    order = np.arange(nx // 2).reshape(north, deep, each).transpose(2, 1, 0).reshape(-1)
    x_high, x_low = left_table(nx)
    rows = max(ROWS, north)
    tx = jnp.asarray(np.stack([stacked(x_high[o], x_low[o]) for o in order.reshape(-1, rows)]))
    order = np.arange(ny).reshape(north, halves, SUB).transpose(1, 0, 2).reshape(-1)
    y_high, y_low = left_table(ny)
    ty = jnp.asarray(stacked(y_high[:, order], y_low[:, order]))
    vmem = pl.BlockSpec(memory_space=pltpu.VMEM)
    smem = pl.BlockSpec(memory_space=pltpu.SMEM)
    chunks = each * halves
    rows = SUB * north
    v = pl.pallas_call(
        functools.partial(kernel, north, deep, each),
        out_shape=jax.ShapeDtypeStruct((deep, each, share_y, kept_z), F32),
        in_specs=[pl.BlockSpec(memory_space=pl.ANY)] + [vmem] * 6 + [smem] * 2 + [vmem],
        out_specs=vmem,
        scratch_shapes=[
            pltpu.VMEM((halves, nx, SUB, nz_part), F32),
            pltpu.VMEM((SUB, 2 * nx, TILE), BF16),
            pltpu.VMEM((each, deep, halves, north, SUB, nz_part), F32),
            pltpu.VMEM((each, deep, halves, north, SUB, nz_part), F32),
            pltpu.VMEM((each, halves, north, SUB, kept_z), F32),
            pltpu.VMEM((each, halves, north, SUB, kept_z), F32),
            pltpu.VMEM((each, deep, share_y, kept_z), F32),
            pltpu.VMEM((deep, each, share_y, kept_z), F32),
            pltpu.VMEM((nz, kept_z), BF16),
            pltpu.VMEM((nz, kept_z), BF16),
            pltpu.VMEM((2 * rows, 2 * nz_part), BF16),
            pltpu.VMEM((rows, 2 * nz_part), BF16),
            pltpu.SemaphoreType.DMA((halves * nz_part // TILE,)),
        ]
        + [
            pltpu.SemaphoreType.DMA((sets, peers))
            for sets, peers in ((2 * chunks, deep), (chunks, north), (2 * each, deep))
            for _ in range(2)
        ],
        compiler_params=pltpu.CompilerParams(
            collective_id=0, has_side_effects=True, vmem_limit_bytes=67043328
        ),
    )(source, tx, ty, *long_tables(nz), symbol_x, symbol_y, symbol_z[None, :])
    return v.reshape(deep * each, share_y, kept_z)


def solution(mesh):
    in_specs = (P(None, "north", "deep"), P(), P(), P())
    out_specs = P("north", "deep", None)
    return jax.shard_map(
        on_device, mesh=mesh, in_specs=in_specs, out_specs=out_specs, check_vma=False
    )
```

```python
import functools

import jax
import jax.numpy as jnp
import numpy as np
from jax import lax
from jax.experimental import pallas as pl
from jax.experimental.pallas import tpu as pltpu
from jax.sharding import PartitionSpec as P

F32, BF16 = jnp.float32, jnp.bfloat16
FINE = 32
TILE = 256
SUB = 8
ROWS = 64


def angles(rows, modes, count):
    rank = np.outer(rows, modes) % (2 * count + 2)
    return np.pi / (count + 1) * rank


def split_np(table):
    high = table.astype(np.float32).astype(BF16)
    low = (table - high.astype(np.float64)).astype(np.float32).astype(BF16)
    return high, low


def left_table(count):
    gain = (2.0 / (count + 1)) ** 0.5
    table = np.sin(angles(np.arange(1, count // 2 + 1), np.arange(1, count + 1), count)) * gain
    return split_np(table)


def stacked(high, low):
    return np.block([[high, high], [low, np.zeros_like(low)]])


def long_tables(count):
    modes = np.arange(1, count // 2 + 1)
    gain = (2.0 / (count + 1)) ** 0.5
    coarse = angles(np.arange(0, count, FINE), modes, count)
    step = angles(np.arange(1, FINE + 1), modes, count)
    f32 = lambda v: jnp.asarray(v.astype(np.float32))
    return f32(np.sin(coarse) * gain), f32(np.cos(coarse) * gain), f32(np.sin(step)), f32(np.cos(step))


def split(values):
    high = values.astype(BF16)
    return high, (values - high.astype(F32)).astype(BF16)


def dot(a, b):
    return jnp.dot(a, b, preferred_element_type=F32)


def loop(count, body):
    if count == 1:
        body(0)
    else:
        lax.fori_loop(0, count, lambda i, c: (body(i), c)[1], 0)


def kernel(
    north, deep, each,
    src, tx_in, ty_in, *rest,
):
    tables_in, (sx_in, sy_in, sz_in, out), scratch = rest[:4], rest[4:8], rest[8:]
    tx, ty, sin_a, cos_a, sin_b, cos_b, symbol_x, symbol_y, symbol_z = scratch[:9]
    field, turned, send1, recv1, send2, recv2, send3, recv3, t_high, t_low, left_all, left = scratch[9:21]
    fs, ins, s1, r1, s2, r2, s3, r3 = scratch[21:]

    me_n, me_d = lax.axis_index("north"), lax.axis_index("deep")
    nx, ny_part, nz_part = src.shape
    halves = ny_part // SUB
    kept_z = t_high.shape[1]
    kept_y = ny_part * north // 2
    share_y = kept_y // deep
    half = north // 2
    pairs = deep // 2
    my_pair = me_d // 2
    far = jnp.where(me_n < half, half, 0)
    bases = (far, half - far)
    last = each - 1
    parts = kept_z // TILE

    loads = {}
    small = []

    def fetch(what, to):
        copy = pltpu.make_async_copy(what, to, ins.at[len(small)])
        copy.start()
        small.append(copy)

    fetch(tx_in, tx)
    for i, (h, c) in enumerate((h, c) for h in range(halves) for c in range(0, nz_part, TILE)):
        loads[h, c] = pltpu.make_async_copy(
            src.at[:, h * SUB : (h + 1) * SUB, c : c + TILE], field.at[h, :, :, c : c + TILE], fs.at[i]
        )
        loads[h, c].start()
    for what, to in zip(
        (*tables_in, ty_in, sx_in, sy_in, sz_in),
        (sin_a, cos_a, sin_b, cos_b, ty, symbol_x, symbol_y, symbol_z),
    ):
        fetch(what, to)

    barrier = pltpu.get_barrier_semaphore()
    for r in range(1, deep):
        pl.semaphore_signal(barrier, inc=1, device_id={"deep": lax.rem(me_d + r, deep)})
    for r in range(1, north):
        pl.semaphore_signal(barrier, inc=1, device_id={"north": lax.rem(me_n + r, north)})

    def x_product(h, c):
        loads[h, c].wait()
        block = min(nx, 128)

        def turn(g):
            for k in range(0, block, 16):
                at = pl.multiple_of(g * block + k, 16)
                high, low = split(jnp.swapaxes(field[h, pl.ds(at, 16), :, c : c + TILE], 0, 1))
                turned[:, pl.ds(at, 16), :] = high
                turned[:, pl.ds(pl.multiple_of(nx + at, 16), 16), :] = low

        loop(nx // block, turn)
        rows = tx.shape[1] // 2
        group = rows // north

        def modes_of(g):
            modes = []
            for y in range(SUB):
                both = dot(tx[g], turned[y])
                modes.append(both[:rows] + both[rows:])
            for k in range(group):
                block = jnp.stack([m[k * north : (k + 1) * north] for m in modes])
                ed = g * group + k
                send1[ed // deep, lax.rem(ed, deep), h, :, :, c : c + TILE] = jnp.swapaxes(block, 0, 1)

        loop(tx.shape[0], modes_of)

    chunks = []
    for f in range(2):
        for e in range(each):
            for h in range(halves):
                cut = half // 2 if not chunks and half % 2 == 0 else half
                chunks += [(f, e, h, i, cut) for i in range(0, half, cut)]

    def copy1(q, r, source):
        f, e, h, i, count = chunks[q]
        at = pl.ds(bases[f] + i, count)
        to = lax.bitwise_xor(me_d, r)
        return pltpu.make_async_remote_copy(
            src_ref=send1.at[e, to, h, at],
            dst_ref=recv1.at[e, source, h, at],
            send_sem=s1.at[q, r],
            recv_sem=r1.at[q, r],
            device_id={"deep": to},
        )

    def send_modes(h_done):
        for q, chunk in enumerate(chunks):
            if (q < half // chunks[0][4]) == (h_done == 0):
                for r in (*range(2, deep), 1):
                    copy1(q, r, me_d).start()

    for h in range(halves):
        for c in range(0, nz_part, TILE):
            if (h, c) == (0, 0):
                small[0].wait()
            x_product(h, c)
        if h == 0:
            pl.semaphore_wait(barrier, deep + north - 2)
            send_modes(0)
    send_modes(1)

    for copy in small[1:]:
        copy.wait()

    def table_step(a):
        table = sin_a[pl.ds(a, 1), :] * cos_b[...] + cos_a[pl.ds(a, 1), :] * sin_b[...]
        high, low = split(table)
        at = pl.multiple_of(a * FINE, FINE)
        t_high[pl.ds(at, FINE), :] = high
        t_low[pl.ds(at, FINE), :] = low

    loop(sin_a.shape[0], table_step)

    def z_product(lhs, count, pair):
        at = pl.multiple_of(pair * 2 * nz_part, 2 * nz_part)
        for c in range(0, kept_z, TILE):
            both = dot(lhs[: 2 * count], t_high[pl.ds(at, 2 * nz_part), c : c + TILE])
            yield c, both[:count] + both[count:] + dot(
                lhs[:count], t_low[pl.ds(at, 2 * nz_part), c : c + TILE]
            )

    def near_part(f, e):
        for q, chunk in enumerate(chunks):
            if chunk[:2] == (f, e):
                copy1(q, 1, lax.bitwise_xor(me_d, 1)).wait_recv()
        at = pl.ds(bases[f], half)
        count = halves * half * SUB
        for owner, block in ((me_d, send1), (lax.bitwise_xor(me_d, 1), recv1)):
            high, low = split(block[e, owner, :, at].reshape(count, nz_part))
            cols = pl.ds(pl.multiple_of(lax.rem(owner, 2) * nz_part, nz_part), nz_part)
            left_all[:count, cols] = high
            left_all[count:, cols] = low
        for c, value in z_product(left_all, count, my_pair):
            value = value.reshape(halves, half, SUB, TILE)
            for h in range(halves):
                send2[e, at, h * SUB : (h + 1) * SUB, c : c + TILE] = value[h]

    def inverse_roots():
        row = lax.broadcasted_iota(jnp.int32, (share_y, TILE), 0)
        part_y = jnp.zeros((share_y, TILE), F32)
        for j in range(share_y):
            part_y = jnp.where(row == j, symbol_y[me_d * share_y + j], part_y)
        for d in range(deep):
            for e in range(each):
                part_x = symbol_x[me_n * deep * each + d * each + e]
                for c in range(0, kept_z, TILE):
                    out[d, e, :, c : c + TILE] = lax.rsqrt(part_x + part_y + symbol_z[:, c : c + TILE])

    def units(e):
        return parts if e == last else halves

    def copy2(e, u, n, source):
        rows = slice(None) if e == last else slice(u * SUB, (u + 1) * SUB)
        cols = slice(u * TILE, (u + 1) * TILE) if e == last else slice(None)
        base = e * halves
        return pltpu.make_async_remote_copy(
            src_ref=send2.at[e, n, rows, cols],
            dst_ref=recv2.at[e, source, rows, cols],
            send_sem=s2.at[base + u, n],
            recv_sem=r2.at[base + u, source],
            device_id={"north": n},
        )

    def every(count, body):
        if count <= 8:
            for i in range(count):
                body(i)
        else:
            loop(count, body)

    def send_north(f, e, u, i, count):
        def one(k):
            n = bases[f] + i + k
            if f == 0:
                copy2(e, u, n, me_n).start()
            else:
                pl.when(n != me_n)(lambda: copy2(e, u, n, me_n).start())

        every(count, one)

    def others(body):
        every(north - 1, lambda r: body(r + jnp.asarray(r >= me_n, jnp.int32)))

    def copy3(e, p, r, owner):
        to = lax.bitwise_xor(me_d, r)
        cols = slice(p * TILE, (p + 1) * TILE) if e == last else slice(None)
        return pltpu.make_async_remote_copy(
            src_ref=send3.at[e, to, :, cols],
            dst_ref=recv3.at[owner, e, :, cols],
            send_sem=s3.at[e + p, r],
            recv_sem=r3.at[e + p, r],
            device_id={"deep": to},
        )

    def y_stage(e, p):
        for u in range(halves) if e < last else (p,):
            others(lambda n: copy2(e, u, n, n).wait_recv())
        for c in range(0, kept_z, TILE) if e < last else (p * TILE,):
            values = recv2[e, :, :, c : c + TILE].reshape(ny_part * north, TILE)
            both = dot(ty[...], jnp.concatenate(split(values), axis=0))
            modes = both[:kept_y] + both[kept_y:]
            send3[e, :, :, c : c + TILE] = modes.reshape(deep, share_y, TILE)
        for r in (*range(2, deep), 1):
            copy3(e, p, r, me_d).start()

    for q, (f, e, h, i, count) in enumerate(chunks):
        if h == 0 and i == 0:
            near_part(f, e)
        rows = count * SUB
        at = pl.ds(bases[f] + i, count)
        for pair in range(1, pairs):
            other = lax.rem(my_pair + pair, pairs)
            for k in range(2):
                owner = other * 2 + k
                r = lax.bitwise_xor(owner, me_d)
                copy1(q, r, owner).wait_recv()
                high, low = split(recv1[e, owner, h, at].reshape(rows, nz_part))
                left[:rows, k * nz_part : (k + 1) * nz_part] = high
                left[rows : 2 * rows, k * nz_part : (k + 1) * nz_part] = low
            for c, value in z_product(left, rows, other):
                send2[e, at, h * SUB : (h + 1) * SUB, c : c + TILE] += value.reshape(count, SUB, TILE)
        if e < last:
            send_north(f, e, h, i, count)
        elif h == halves - 1:
            for u in range(parts):
                send_north(f, e, u, 0, half)
        if q == 0:
            inverse_roots()

    for e in range(each):
        recv2[e, me_n] = send2[e, me_n]
    for e in range(each):
        for p in range(parts if e == last else 1):
            y_stage(e, p)

    for q in range(len(chunks)):
        for r in range(1, deep):
            copy1(q, r, me_d).wait_send()
    for e in range(each):
        for u in range(units(e)):
            others(lambda n: copy2(e, u, n, me_n).wait_send())
    for e in range(each):
        out[me_d, e] = out[me_d, e] * send3[e, me_d]
        for p in range(parts if e == last else 1):
            cols = slice(p * TILE, (p + 1) * TILE) if e == last else slice(None)
            for r in range(1, deep):
                owner = lax.bitwise_xor(me_d, r)
                copy = copy3(e, p, r, owner)
                copy.wait_recv()
                out[owner, e, :, cols] = out[owner, e, :, cols] * recv3[owner, e, :, cols]
                copy.wait_send()


def on_device(source, symbol_x, symbol_y, symbol_z):
    north, deep = lax.axis_size("north"), lax.axis_size("deep")
    nx, ny_part, nz_part = source.shape
    each, halves = nx // 2 // north // deep, ny_part // SUB
    ny, nz = ny_part * north, nz_part * deep
    kept_z, share_y = nz // 2, ny // 2 // deep
    order = np.arange(nx // 2).reshape(north, deep, each).transpose(2, 1, 0).reshape(-1)
    x_high, x_low = left_table(nx)
    rows = max(ROWS, north)
    tx = jnp.asarray(np.stack([stacked(x_high[o], x_low[o]) for o in order.reshape(-1, rows)]))
    ty = jnp.asarray(stacked(*left_table(ny)))
    tables = long_tables(nz)
    anywhere = pl.BlockSpec(memory_space=pl.ANY)
    rows = SUB * north
    chunks = 2 * each * halves + 1
    operands = (source, tx, ty, *tables, symbol_x, symbol_y, symbol_z[None, :])
    v = pl.pallas_call(
        functools.partial(kernel, north, deep, each),
        out_shape=jax.ShapeDtypeStruct((deep, each, share_y, kept_z), F32),
        in_specs=[anywhere] * len(operands),
        out_specs=pl.BlockSpec(memory_space=pltpu.VMEM),
        scratch_shapes=[pltpu.VMEM(t.shape, t.dtype) for t in (tx, ty, *tables)]
        + [
            pltpu.SMEM(symbol_x.shape, F32),
            pltpu.SMEM(symbol_y.shape, F32),
            pltpu.VMEM((1, nz), F32),
            pltpu.VMEM((halves, nx, SUB, nz_part), F32),
            pltpu.VMEM((SUB, 2 * nx, TILE), BF16),
            pltpu.VMEM((each, deep, halves, north, SUB, nz_part), F32),
            pltpu.VMEM((each, deep, halves, north, SUB, nz_part), F32),
            pltpu.VMEM((each, north, ny_part, kept_z), F32),
            pltpu.VMEM((each, north, ny_part, kept_z), F32),
            pltpu.VMEM((each, deep, share_y, kept_z), F32),
            pltpu.VMEM((deep, each, share_y, kept_z), F32),
            pltpu.VMEM((nz, kept_z), BF16),
            pltpu.VMEM((nz, kept_z), BF16),
            pltpu.VMEM((halves * rows, 2 * nz_part), BF16),
            pltpu.VMEM((rows, 2 * nz_part), BF16),
            pltpu.SemaphoreType.DMA((halves * nz_part // TILE,)),
            pltpu.SemaphoreType.DMA((len(operands),)),
        ]
        + [
            pltpu.SemaphoreType.DMA((sets, peers))
            for sets, peers in (
                (chunks, deep),
                (each * halves + kept_z // TILE, north),
                (each + kept_z // TILE, deep),
            )
            for _ in range(2)
        ],
        compiler_params=pltpu.CompilerParams(
            collective_id=0, has_side_effects=True, vmem_limit_bytes=67043328
        ),
    )(*operands)
    return v.reshape(deep * each, share_y, kept_z)


def solution(mesh):
    in_specs = (P(None, "north", "deep"), P(), P(), P())
    out_specs = P("north", "deep", None)
    return jax.shard_map(
        on_device, mesh=mesh, in_specs=in_specs, out_specs=out_specs, check_vma=False
    )
```

```python
import functools

import jax
import jax.numpy as jnp
import numpy as np
from jax import lax
from jax.experimental import pallas as pl
from jax.experimental.pallas import tpu as pltpu
from jax.sharding import PartitionSpec as P

F32, BF16 = jnp.float32, jnp.bfloat16
FINE = 32
TILE = 256
SUB = 8
ROWS = 64


def angles(rows, modes, count):
    rank = np.outer(rows, modes) % (2 * count + 2)
    return np.pi / (count + 1) * rank


def split_np(table):
    high = table.astype(np.float32).astype(BF16)
    low = (table - high.astype(np.float64)).astype(np.float32).astype(BF16)
    return high, low


def left_table(count):
    gain = (2.0 / (count + 1)) ** 0.5
    table = np.sin(angles(np.arange(1, count // 2 + 1), np.arange(1, count + 1), count)) * gain
    return split_np(table)


def stacked(high, low):
    return np.block([[high, high], [low, np.zeros_like(low)]])


def long_tables(count):
    modes = np.arange(1, count // 2 + 1)
    gain = (2.0 / (count + 1)) ** 0.5
    coarse = angles(np.arange(0, count, FINE), modes, count)
    step = angles(np.arange(1, FINE + 1), modes, count)
    parts = (np.sin(coarse) * gain, np.cos(coarse) * gain, np.sin(step), np.cos(step))
    return jnp.asarray(np.concatenate(parts).astype(np.float32))


def split(values):
    high = values.astype(BF16)
    return high, (values - high.astype(F32)).astype(BF16)


def dot(a, b):
    return jnp.dot(a, b, preferred_element_type=F32)


def loop(count, body):
    if count == 1:
        body(0)
    else:
        lax.fori_loop(0, count, lambda i, c: (body(i), c)[1], 0)


def kernel(
    north, deep, each,
    src, tx_in, ty_in, *rest,
):
    waves_in, sx_in, sy_in, sz_in, out = rest[:5]
    tx, ty, waves, symbol_x, symbol_y, symbol_z = rest[5:11]
    field, turned, send1, recv1, send2, recv2, send3, recv3, t_high, t_low, left_all, left = rest[11:23]
    fs, ins, sent, r1, r2, r3 = rest[23:]

    me_n, me_d = lax.axis_index("north"), lax.axis_index("deep")
    nx, ny_part, nz_part = src.shape
    halves = ny_part // SUB
    kept_z = t_high.shape[1]
    kept_y = ny_part * north // 2
    share_y = kept_y // deep
    half = north // 2
    pairs = deep // 2
    my_pair = me_d // 2
    far = jnp.where(me_n < half, half, 0)
    bases = (far, half - far)
    last = each - 1
    parts = kept_z // TILE

    loads = {}
    small = []

    def fetch(what, to):
        copy = pltpu.make_async_copy(what, to, ins.at[len(small)])
        copy.start()
        small.append(copy)

    fetch(tx_in, tx)
    for i, (h, c) in enumerate((h, c) for h in range(halves) for c in range(0, nz_part, TILE)):
        loads[h, c] = pltpu.make_async_copy(
            src.at[:, h * SUB : (h + 1) * SUB, c : c + TILE], field.at[h, :, :, c : c + TILE], fs.at[i]
        )
        loads[h, c].start()
    for what, to in zip(
        (waves_in, ty_in, sx_in, sy_in, sz_in),
        (waves, ty, symbol_x, symbol_y, symbol_z),
    ):
        fetch(what, to)

    barrier = pltpu.get_barrier_semaphore()
    for r in range(1, deep):
        pl.semaphore_signal(barrier, inc=1, device_id={"deep": lax.rem(me_d + r, deep)})
    for r in range(1, north):
        pl.semaphore_signal(barrier, inc=1, device_id={"north": lax.rem(me_n + r, north)})

    def x_product(h, c):
        loads[h, c].wait()
        block = min(nx, 128)

        def turn(g):
            for k in range(0, block, 16):
                at = pl.multiple_of(g * block + k, 16)
                high, low = split(jnp.swapaxes(field[h, pl.ds(at, 16), :, c : c + TILE], 0, 1))
                turned[:, pl.ds(at, 16), :] = high
                turned[:, pl.ds(pl.multiple_of(nx + at, 16), 16), :] = low

        loop(nx // block, turn)
        rows = tx.shape[1] // 2
        group = rows // north

        def modes_of(g):
            modes = []
            for y in range(SUB):
                both = dot(tx[g], turned[y])
                modes.append(both[:rows] + both[rows:])
            for k in range(group):
                block = jnp.stack([m[k * north : (k + 1) * north] for m in modes])
                ed = g * group + k
                send1[ed // deep, lax.rem(ed, deep), h, :, :, c : c + TILE] = jnp.swapaxes(block, 0, 1)

        loop(tx.shape[0], modes_of)

    chunks = []
    for f in range(2):
        for e in range(each):
            for h in range(halves):
                cut = half // 2 if not chunks and half % 2 == 0 else half
                chunks += [(f, e, h, i, cut) for i in range(0, half, cut)]

    def copy1(q, r):
        f, e, h, i, count = chunks[q]
        at = pl.ds(bases[f] + i, count)
        to = lax.bitwise_xor(me_d, r)
        key = 2 * each * halves + 1 + f * each + e if r == 1 else q
        return pltpu.make_async_remote_copy(
            src_ref=send1.at[e, to, h, at],
            dst_ref=recv1.at[e, me_d, h, at],
            send_sem=sent.at[0],
            recv_sem=r1.at[key],
            device_id={"deep": to},
        )

    def send_modes(h_done):
        for q, chunk in enumerate(chunks):
            if (q < half // chunks[0][4]) == (h_done == 0):
                for r in (*range(2, deep), 1):
                    copy1(q, r).start()

    for h in range(halves):
        for c in range(0, nz_part, TILE):
            if (h, c) == (0, 0):
                small[0].wait()
            x_product(h, c)
        if h == 0:
            pl.semaphore_wait(barrier, deep + north - 2)
            send_modes(0)
    send_modes(1)

    for copy in small[1:]:
        copy.wait()

    coarse = waves.shape[0] // 2 - FINE

    def table_step(a):
        sin_a, cos_a = waves[pl.ds(a, 1), :], waves[pl.ds(coarse + a, 1), :]
        table = sin_a * waves[2 * coarse + FINE :, :] + cos_a * waves[2 * coarse : 2 * coarse + FINE, :]
        high, low = split(table)
        at = pl.multiple_of(a * FINE, FINE)
        t_high[pl.ds(at, FINE), :] = high
        t_low[pl.ds(at, FINE), :] = low

    loop(coarse, table_step)

    def z_product(lhs, count, pair):
        at = pl.multiple_of(pair * 2 * nz_part, 2 * nz_part)
        for c in range(0, kept_z, TILE):
            both = dot(lhs[: 2 * count], t_high[pl.ds(at, 2 * nz_part), c : c + TILE])
            yield c, both[:count] + both[count:] + dot(
                lhs[:count], t_low[pl.ds(at, 2 * nz_part), c : c + TILE]
            )

    def near_part(f, e):
        at = pl.ds(bases[f], half)
        block = recv1.at[e, lax.bitwise_xor(me_d, 1), :, at]
        pltpu.make_async_copy(block, block, r1.at[2 * each * halves + 1 + f * each + e]).wait()
        count = halves * half * SUB
        for owner, block in ((me_d, send1), (lax.bitwise_xor(me_d, 1), recv1)):
            high, low = split(block[e, owner, :, at].reshape(count, nz_part))
            cols = pl.ds(pl.multiple_of(lax.rem(owner, 2) * nz_part, nz_part), nz_part)
            left_all[:count, cols] = high
            left_all[count:, cols] = low
        for c, value in z_product(left_all, count, my_pair):
            value = value.reshape(halves, half, SUB, TILE)
            for h in range(halves):
                send2[e, at, h * SUB : (h + 1) * SUB, c : c + TILE] = value[h]

    def inverse_roots():
        row = lax.broadcasted_iota(jnp.int32, (share_y, TILE), 0)
        part_y = jnp.zeros((share_y, TILE), F32)
        for j in range(share_y):
            part_y = jnp.where(row == j, symbol_y[me_d * share_y + j], part_y)
        for d in range(deep):
            for e in range(each):
                part_x = symbol_x[me_n * deep * each + d * each + e]
                for c in range(0, kept_z, TILE):
                    out[d, e, :, c : c + TILE] = lax.rsqrt(part_x + part_y + symbol_z[:, c : c + TILE])

    def units(e):
        return parts if e == last else halves

    def copy2(e, u, n):
        rows = slice(None) if e == last else slice(u * SUB, (u + 1) * SUB)
        cols = slice(u * TILE, (u + 1) * TILE) if e == last else slice(None)
        return pltpu.make_async_remote_copy(
            src_ref=send2.at[e, n, rows, cols],
            dst_ref=recv2.at[e, me_n, rows, cols],
            send_sem=sent.at[1],
            recv_sem=r2.at[e + u if e == last else e],
            device_id={"north": n},
        )

    def every(count, body):
        if count <= 8:
            for i in range(count):
                body(i)
        else:
            loop(count, body)

    def send_north(f, e, u, i, count):
        def one(k):
            n = bases[f] + i + k
            if f == 0:
                copy2(e, u, n).start()
            else:
                pl.when(n != me_n)(lambda: copy2(e, u, n).start())

        every(count, one)

    def copy3(e, p, r):
        to = lax.bitwise_xor(me_d, r)
        cols = slice(p * TILE, (p + 1) * TILE) if e == last else slice(None)
        return pltpu.make_async_remote_copy(
            src_ref=send3.at[e, to, :, cols],
            dst_ref=recv3.at[me_d, e, :, cols],
            send_sem=sent.at[2],
            recv_sem=r3.at[e + p],
            device_id={"deep": to},
        )

    def y_stage(e, p):
        cols = slice(p * TILE, (p + 1) * TILE) if e == last else slice(None)
        block = recv2.at[e, pl.ds(0, north - 1), :, cols]
        pltpu.make_async_copy(block, block, r2.at[e + p]).wait()
        for c in range(0, kept_z, TILE) if e < last else (p * TILE,):
            values = recv2[e, :, :, c : c + TILE].reshape(ny_part * north, TILE)
            both = dot(ty[...], jnp.concatenate(split(values), axis=0))
            modes = both[:kept_y] + both[kept_y:]
            send3[e, :, :, c : c + TILE] = modes.reshape(deep, share_y, TILE)
        for r in (*range(2, deep), 1):
            copy3(e, p, r).start()

    for q, (f, e, h, i, count) in enumerate(chunks):
        if h == 0 and i == 0:
            near_part(f, e)
        rows = count * SUB
        at = pl.ds(bases[f] + i, count)
        for pair in range(1, pairs):
            other = lax.rem(my_pair + pair, pairs)
            block = recv1.at[e, pl.ds(other * 2, 2), h, at]
            pltpu.make_async_copy(block, block, r1.at[q]).wait()
            for k in range(2):
                owner = other * 2 + k
                high, low = split(recv1[e, owner, h, at].reshape(rows, nz_part))
                left[:rows, k * nz_part : (k + 1) * nz_part] = high
                left[rows : 2 * rows, k * nz_part : (k + 1) * nz_part] = low
            for c, value in z_product(left, rows, other):
                send2[e, at, h * SUB : (h + 1) * SUB, c : c + TILE] += value.reshape(count, SUB, TILE)
        if e < last:
            send_north(f, e, h, i, count)
        elif h == halves - 1:
            for u in range(parts):
                send_north(f, e, u, 0, half)
        if q == 0:
            inverse_roots()

    for e in range(each):
        recv2[e, me_n] = send2[e, me_n]
    for e in range(each):
        for p in range(parts if e == last else 1):
            y_stage(e, p)

    for e in range(each):
        out[me_d, e] = out[me_d, e] * send3[e, me_d]
        for p in range(parts if e == last else 1):
            cols = slice(p * TILE, (p + 1) * TILE) if e == last else slice(None)
            block = recv3.at[pl.ds(0, deep - 1), e, :, cols]
            pltpu.make_async_copy(block, block, r3.at[e + p]).wait()
            for r in range(1, deep):
                owner = lax.bitwise_xor(me_d, r)
                out[owner, e, :, cols] = out[owner, e, :, cols] * recv3[owner, e, :, cols]
    for i, block in enumerate((
        send1.at[:, pl.ds(0, deep - 1)],
        send2.at[:, pl.ds(0, north - 1)],
        send3.at[:, pl.ds(0, deep - 1)],
    )):
        pltpu.make_async_copy(block, block, sent.at[i]).wait()


def on_device(source, symbol_x, symbol_y, symbol_z):
    north, deep = lax.axis_size("north"), lax.axis_size("deep")
    nx, ny_part, nz_part = source.shape
    each, halves = nx // 2 // north // deep, ny_part // SUB
    ny, nz = ny_part * north, nz_part * deep
    kept_z, share_y = nz // 2, ny // 2 // deep
    order = np.arange(nx // 2).reshape(north, deep, each).transpose(2, 1, 0).reshape(-1)
    x_high, x_low = left_table(nx)
    rows = max(ROWS, north)
    tx = jnp.asarray(np.stack([stacked(x_high[o], x_low[o]) for o in order.reshape(-1, rows)]))
    ty = jnp.asarray(stacked(*left_table(ny)))
    waves = long_tables(nz)
    remote = pl.BlockSpec(memory_space=pltpu.HBM)
    rows = SUB * north
    chunks = 2 * each * halves + 1
    operands = (source, tx, ty, waves, symbol_x, symbol_y, symbol_z[None, :])
    v = pl.pallas_call(
        functools.partial(kernel, north, deep, each),
        out_shape=jax.ShapeDtypeStruct((deep, each, share_y, kept_z), F32),
        in_specs=[remote] * len(operands),
        out_specs=pl.BlockSpec(memory_space=pltpu.VMEM),
        scratch_shapes=[pltpu.VMEM(t.shape, t.dtype) for t in (tx, ty, waves)]
        + [
            pltpu.SMEM(symbol_x.shape, F32),
            pltpu.SMEM(symbol_y.shape, F32),
            pltpu.VMEM((1, nz), F32),
            pltpu.VMEM((halves, nx, SUB, nz_part), F32),
            pltpu.VMEM((SUB, 2 * nx, TILE), BF16),
            pltpu.VMEM((each, deep, halves, north, SUB, nz_part), F32),
            pltpu.VMEM((each, deep, halves, north, SUB, nz_part), F32),
            pltpu.VMEM((each, north, ny_part, kept_z), F32),
            pltpu.VMEM((each, north, ny_part, kept_z), F32),
            pltpu.VMEM((each, deep, share_y, kept_z), F32),
            pltpu.VMEM((deep, each, share_y, kept_z), F32),
            pltpu.VMEM((nz, kept_z), BF16),
            pltpu.VMEM((nz, kept_z), BF16),
            pltpu.VMEM((halves * rows, 2 * nz_part), BF16),
            pltpu.VMEM((rows, 2 * nz_part), BF16),
            pltpu.SemaphoreType.DMA((halves * nz_part // TILE,)),
            pltpu.SemaphoreType.DMA((len(operands) - 1,)),
        ]
        + [
            pltpu.SemaphoreType.DMA((count,))
            for count in (3, chunks + 2 * each, each + kept_z // TILE, each + kept_z // TILE)
        ],
        compiler_params=pltpu.CompilerParams(
            collective_id=0, has_side_effects=True, vmem_limit_bytes=67043328
        ),
    )(*operands)
    return v.reshape(deep * each, share_y, kept_z)


def solution(mesh):
    in_specs = (P(None, "north", "deep"), P(), P(), P())
    out_specs = P("north", "deep", None)
    return jax.shard_map(
        on_device, mesh=mesh, in_specs=in_specs, out_specs=out_specs, check_vma=False
    )
```

```python
import functools

import jax
import jax.numpy as jnp
import numpy as np
from jax import lax
from jax.experimental import pallas as pl
from jax.experimental.pallas import tpu as pltpu
from jax.sharding import PartitionSpec as P

F32, BF16 = jnp.float32, jnp.bfloat16
FINE = 32
TILE = 256
SUB = 8
ROWS = 64
MOST = 67043328
SPARE = 14 << 20


def angles(rows, modes, count):
    rank = np.outer(rows, modes) % (2 * count + 2)
    return np.pi / (count + 1) * rank


def split_np(table):
    high = table.astype(np.float32).astype(BF16)
    low = (table - high.astype(np.float64)).astype(np.float32).astype(BF16)
    return high, low


def left_table(count):
    gain = (2.0 / (count + 1)) ** 0.5
    table = np.sin(angles(np.arange(1, count // 2 + 1), np.arange(1, count + 1), count)) * gain
    return split_np(table)


def stacked(high, low):
    return np.block([[high, high], [low, np.zeros_like(low)]])


def long_tables(count):
    modes = np.arange(1, count // 2 + 1)
    gain = (2.0 / (count + 1)) ** 0.5
    coarse = angles(np.arange(0, count, FINE), modes, count)
    step = angles(np.arange(1, FINE + 1), modes, count)
    parts = (np.sin(coarse) * gain, np.cos(coarse) * gain, np.sin(step), np.cos(step))
    return jnp.asarray(np.concatenate(parts).astype(np.float32))


def split(values):
    high = values.astype(BF16)
    return high, (values - high.astype(F32)).astype(BF16)


def dot(a, b):
    return jnp.dot(a, b, preferred_element_type=F32)


def loop(count, body):
    if count == 1:
        body(0)
    else:
        lax.fori_loop(0, count, lambda i, c: (body(i), c)[1], 0)


def kernel(
    north, deep, each,
    src, tx_in, ty_in, *rest,
):
    waves_in, sx_in, sy_in, sz_in, out = rest[:5]
    tx, ty, waves, symbol_z = rest[5:9]
    field, turned, send1, recv1, send2, recv2, send3, recv3, t_high, t_low, left_all, left = rest[9:21]
    symbol_x, symbol_y, fs, ins, sent, r1, r2, r3 = rest[21:]

    me_n, me_d = lax.axis_index("north"), lax.axis_index("deep")
    nx, ny_part, nz_part = src.shape
    halves = ny_part // SUB
    kept_z = t_high.shape[1]
    kept_y = ny_part * north // 2
    share_y = kept_y // deep
    half = north // 2
    pairs = deep // 2
    my_pair = me_d // 2
    far = jnp.where(me_n < half, half, 0)
    bases = (far, half - far)
    last = each - 1
    parts = kept_z // TILE

    loads = {}
    small = []

    def fetch(what, to):
        copy = pltpu.make_async_copy(what, to, ins.at[len(small)])
        copy.start()
        small.append(copy)

    fetch(tx_in, tx)
    for i, (h, c) in enumerate((h, c) for h in range(halves) for c in range(0, nz_part, TILE)):
        loads[h, c] = pltpu.make_async_copy(
            src.at[:, h * SUB : (h + 1) * SUB, c : c + TILE], field.at[h, :, :, c : c + TILE], fs.at[i]
        )
        loads[h, c].start()
    for what, to in zip(
        (waves_in, ty_in, sx_in, sy_in, sz_in),
        (waves, ty, symbol_x, symbol_y, symbol_z),
    ):
        fetch(what, to)

    barrier = pltpu.get_barrier_semaphore()
    for r in range(1, deep):
        pl.semaphore_signal(barrier, inc=1, device_id={"deep": lax.rem(me_d + r, deep)})
    for r in range(1, north):
        pl.semaphore_signal(barrier, inc=1, device_id={"north": lax.rem(me_n + r, north)})

    def x_product(h, c):
        loads[h, c].wait()
        block = min(nx, 128)

        def turn(g):
            for k in range(0, block, 16):
                at = pl.multiple_of(g * block + k, 16)
                high, low = split(jnp.swapaxes(field[h, pl.ds(at, 16), :, c : c + TILE], 0, 1))
                turned[:, pl.ds(at, 16), :] = high
                turned[:, pl.ds(pl.multiple_of(nx + at, 16), 16), :] = low

        loop(nx // block, turn)
        rows = tx.shape[1] // 2
        group = rows // north

        def modes_of(g):
            modes = []
            for y in range(SUB):
                both = dot(tx[g], turned[y])
                modes.append(both[:rows] + both[rows:])
            for k in range(group):
                block = jnp.stack([m[k * north : (k + 1) * north] for m in modes])
                ed = g * group + k
                send1[ed // deep, lax.rem(ed, deep), h, :, :, c : c + TILE] = jnp.swapaxes(block, 0, 1)

        loop(tx.shape[0], modes_of)

    chunks = []
    for f in range(2):
        for e in range(each):
            for h in range(halves):
                cut = half // 2 if not chunks and half % 2 == 0 else half
                chunks += [(f, e, h, i, cut) for i in range(0, half, cut)]

    def copy1(q, r):
        f, e, h, i, count = chunks[q]
        at = pl.ds(bases[f] + i, count)
        to = lax.bitwise_xor(me_d, r)
        key = 2 * each * halves + 1 + f * each + e if r == 1 else q
        return pltpu.make_async_remote_copy(
            src_ref=send1.at[e, to, h, at],
            dst_ref=recv1.at[e, me_d, h, at],
            send_sem=sent.at[0],
            recv_sem=r1.at[key],
            device_id={"deep": to},
        )

    def send_modes(h_done):
        for q, chunk in enumerate(chunks):
            if (q < half // chunks[0][4]) == (h_done == 0):
                for r in (*range(2, deep), 1):
                    copy1(q, r).start()

    for h in range(halves):
        for c in range(0, nz_part, TILE):
            if (h, c) == (0, 0):
                small[0].wait()
            x_product(h, c)
        if h == 0:
            pl.semaphore_wait(barrier, deep + north - 2)
            send_modes(0)
    send_modes(1)

    for copy in small[1:]:
        copy.wait()

    coarse = waves.shape[0] // 2 - FINE

    def table_tile(c):
        cols = slice(c, c + TILE)
        cos_b = waves[2 * coarse + FINE :, cols]
        sin_b = waves[2 * coarse : 2 * coarse + FINE, cols]

        def table_step(g):
            for k in range(4):
                a = g * 4 + k
                table = waves[pl.ds(a, 1), cols] * cos_b + waves[pl.ds(coarse + a, 1), cols] * sin_b
                high, low = split(table)
                at = pl.multiple_of(a * FINE, FINE)
                t_high[pl.ds(at, FINE), cols] = high
                t_low[pl.ds(at, FINE), cols] = low

        loop(coarse // 4, table_step)

    tiles = range(0, kept_z, TILE)

    def z_tile(lhs, count, pair, c):
        at = pl.ds(pl.multiple_of(pair * 2 * nz_part, 2 * nz_part), 2 * nz_part)
        both = dot(lhs[: 2 * count], t_high[at, c : c + TILE])
        return both[:count] + both[count:] + dot(lhs[:count], t_low[at, c : c + TILE])

    def near_left(f, e):
        at = pl.ds(bases[f], half)
        block = recv1.at[e, lax.bitwise_xor(me_d, 1), :, at]
        pltpu.make_async_copy(block, block, r1.at[2 * each * halves + 1 + f * each + e]).wait()
        count = halves * half * SUB
        for owner, block in ((me_d, send1), (lax.bitwise_xor(me_d, 1), recv1)):
            high, low = split(block[e, owner, :, at].reshape(count, nz_part))
            cols = pl.ds(pl.multiple_of(lax.rem(owner, 2) * nz_part, nz_part), nz_part)
            left_all[:count, cols] = high
            left_all[count:, cols] = low

    def near_tile(f, e, c):
        value = z_tile(left_all, halves * half * SUB, my_pair, c).reshape(halves, half, SUB, TILE)
        for h in range(halves):
            send2[e, pl.ds(bases[f], half), h * SUB : (h + 1) * SUB, c : c + TILE] = value[h]

    def far_left(q, pair):
        f, e, h, i, count = chunks[q]
        at, rows = pl.ds(bases[f] + i, count), count * SUB
        block = recv1.at[e, pl.ds(pair * 2, 2), h, at]
        pltpu.make_async_copy(block, block, r1.at[q]).wait()
        for k in range(2):
            high, low = split(recv1[e, pair * 2 + k, h, at].reshape(rows, nz_part))
            left[:rows, k * nz_part : (k + 1) * nz_part] = high
            left[rows : 2 * rows, k * nz_part : (k + 1) * nz_part] = low

    def far_tile(q, pair, c):
        f, e, h, i, count = chunks[q]
        value = z_tile(left, count * SUB, pair, c).reshape(count, SUB, TILE)
        send2[e, pl.ds(bases[f] + i, count), h * SUB : (h + 1) * SUB, c : c + TILE] += value

    def inverse_roots():
        row = lax.broadcasted_iota(jnp.int32, (share_y, TILE), 0)
        part_y = jnp.zeros((share_y, TILE), F32)
        for j in range(share_y):
            part_y = jnp.where(row == j, symbol_y[me_d * share_y + j], part_y)
        for d in range(deep):
            for e in range(each):
                part_x = symbol_x[me_n * deep * each + d * each + e]
                for c in range(0, kept_z, TILE):
                    out[d, e, :, c : c + TILE] = lax.rsqrt(part_x + part_y + symbol_z[:, c : c + TILE])

    def copy2(e, rows, cols, n):
        return pltpu.make_async_remote_copy(
            src_ref=send2.at[e, n, rows, cols],
            dst_ref=recv2.at[e, me_n, rows, cols],
            send_sem=sent.at[1],
            recv_sem=r2.at[e + (cols.start // TILE if e == last else 0)],
            device_id={"north": n},
        )

    def every(count, body):
        if count <= 8:
            for i in range(count):
                body(i)
        else:
            loop(count, body)

    def send_north(f, e, rows, cols, n):
        if f == 0:
            copy2(e, rows, cols, n).start()
        else:
            pl.when(n != me_n)(lambda: copy2(e, rows, cols, n).start())

    def copy3(e, p, r):
        to = lax.bitwise_xor(me_d, r)
        cols = slice(p * TILE, (p + 1) * TILE) if e == last else slice(None)
        return pltpu.make_async_remote_copy(
            src_ref=send3.at[e, to, :, cols],
            dst_ref=recv3.at[me_d, e, :, cols],
            send_sem=sent.at[2],
            recv_sem=r3.at[e + p],
            device_id={"deep": to},
        )

    def y_stage(e, p):
        cols = slice(p * TILE, (p + 1) * TILE) if e == last else slice(None)
        block = recv2.at[e, pl.ds(0, north - 1), :, cols]
        pltpu.make_async_copy(block, block, r2.at[e + p]).wait()
        for c in range(0, kept_z, TILE) if e < last else (p * TILE,):
            values = recv2[e, :, :, c : c + TILE].reshape(ny_part * north, TILE)
            both = dot(ty[...], jnp.concatenate(split(values), axis=0))
            modes = both[:kept_y] + both[kept_y:]
            send3[e, :, :, c : c + TILE] = modes.reshape(deep, share_y, TILE)
        for r in (*range(2, deep), 1):
            copy3(e, p, r).start()

    rivals = [lax.rem(my_pair + k, pairs) for k in range(1, pairs)]
    whole = slice(0, kept_z)
    for q, (f, e, h, i, count) in enumerate(chunks):
        lines = slice(h * SUB, (h + 1) * SUB)
        if q == 0:
            for c in tiles:
                table_tile(c)
                if c == 0:
                    near_left(f, e)
                near_tile(f, e, c)
                if len(rivals) == 1:
                    if c == 0:
                        far_left(q, rivals[0])
                    far_tile(q, rivals[0], c)
                    if e < last:
                        every(count, lambda k: send_north(f, e, lines, slice(c, c + TILE), bases[f] + i + k))
            inverse_roots()
            if len(rivals) == 1:
                continue
        elif h == 0 and i == 0:
            near_left(f, e)
            for c in tiles:
                near_tile(f, e, c)
        for pair in rivals:
            far_left(q, pair)
            for c in tiles:
                far_tile(q, pair, c)
        if e < last:
            every(count, lambda k: send_north(f, e, lines, whole, bases[f] + i + k))
        elif h == halves - 1:
            order = sorted((u - (n == 0), n, u) for u in range(parts) for n in range(half))
            for _, n, u in order:
                send_north(f, e, slice(0, ny_part), slice(u * TILE, (u + 1) * TILE), bases[f] + n)

    for e in range(each):
        recv2[e, me_n] = send2[e, me_n]
    for e in range(each):
        for p in range(parts if e == last else 1):
            y_stage(e, p)

    for e in range(each):
        out[me_d, e] = out[me_d, e] * send3[e, me_d]
        for p in range(parts if e == last else 1):
            cols = slice(p * TILE, (p + 1) * TILE) if e == last else slice(None)
            block = recv3.at[pl.ds(0, deep - 1), e, :, cols]
            pltpu.make_async_copy(block, block, r3.at[e + p]).wait()
            for r in range(1, deep):
                owner = lax.bitwise_xor(me_d, r)
                out[owner, e, :, cols] = out[owner, e, :, cols] * recv3[owner, e, :, cols]
    for i, block in enumerate((
        send1.at[:, pl.ds(0, deep - 1)],
        send2.at[:, pl.ds(0, north - 1)],
        send3.at[:, pl.ds(0, deep - 1)],
    )):
        pltpu.make_async_copy(block, block, sent.at[i]).wait()


def on_device(source, symbol_x, symbol_y, symbol_z):
    north, deep = lax.axis_size("north"), lax.axis_size("deep")
    nx, ny_part, nz_part = source.shape
    each, halves = nx // 2 // north // deep, ny_part // SUB
    ny, nz = ny_part * north, nz_part * deep
    kept_z, share_y = nz // 2, ny // 2 // deep
    order = np.arange(nx // 2).reshape(north, deep, each).transpose(2, 1, 0).reshape(-1)
    x_high, x_low = left_table(nx)
    rows = max(ROWS, north)
    tx = jnp.asarray(np.stack([stacked(x_high[o], x_low[o]) for o in order.reshape(-1, rows)]))
    ty = jnp.asarray(stacked(*left_table(ny)))
    waves = long_tables(nz)
    remote = pl.BlockSpec(memory_space=pltpu.HBM)
    rows = SUB * north
    chunks = 2 * each * halves + 1
    operands = (source, tx, ty, waves, symbol_x, symbol_y, symbol_z[None, :])
    buffers = [
        *((t.shape, t.dtype) for t in (tx, ty, waves)),
        ((1, nz), F32),
        ((halves, nx, SUB, nz_part), F32),
        ((SUB, 2 * nx, TILE), BF16),
        ((each, deep, halves, north, SUB, nz_part), F32),
        ((each, deep, halves, north, SUB, nz_part), F32),
        ((each, north, ny_part, kept_z), F32),
        ((each, north, ny_part, kept_z), F32),
        ((each, deep, share_y, kept_z), F32),
        ((deep, each, share_y, kept_z), F32),
        ((nz, kept_z), BF16),
        ((nz, kept_z), BF16),
        ((halves * rows, 2 * nz_part), BF16),
        ((rows, 2 * nz_part), BF16),
    ]
    used = sum(int(np.prod(shape)) * jnp.dtype(kind).itemsize for shape, kind in buffers)
    limit = MOST - SPARE if used < MOST - 2 * SPARE else MOST
    v = pl.pallas_call(
        functools.partial(kernel, north, deep, each),
        out_shape=jax.ShapeDtypeStruct((deep, each, share_y, kept_z), F32),
        in_specs=[remote] * len(operands),
        out_specs=pl.BlockSpec(memory_space=pltpu.VMEM),
        scratch_shapes=[pltpu.VMEM(shape, kind) for shape, kind in buffers]
        + [
            pltpu.SMEM(symbol_x.shape, F32),
            pltpu.SMEM(symbol_y.shape, F32),
            pltpu.SemaphoreType.DMA((halves * nz_part // TILE,)),
            pltpu.SemaphoreType.DMA((len(operands) - 1,)),
        ]
        + [
            pltpu.SemaphoreType.DMA((count,))
            for count in (3, chunks + 2 * each, each + kept_z // TILE, each + kept_z // TILE)
        ],
        compiler_params=pltpu.CompilerParams(
            collective_id=0, has_side_effects=True, vmem_limit_bytes=limit
        ),
    )(*(pltpu.with_memory_space_constraint(operand, pltpu.HBM) for operand in operands))
    return v.reshape(deep * each, share_y, kept_z)


def solution(mesh):
    in_specs = (P(None, "north", "deep"), P(), P(), P())
    out_specs = P("north", "deep", None)
    return jax.shard_map(
        on_device, mesh=mesh, in_specs=in_specs, out_specs=out_specs, check_vma=False
    )
```

```python
import functools

import jax
import jax.numpy as jnp
import numpy as np
from jax import lax
from jax.experimental import pallas as pl
from jax.experimental.pallas import tpu as pltpu
from jax.sharding import PartitionSpec as P

F32, BF16 = jnp.float32, jnp.bfloat16
FINE = 32
TILE = 256
WIDE = 512
SUB = 8
ROWS = 64
MOST = 67043328
SPARE = 14 << 20


def angles(rows, modes, count):
    rank = np.outer(rows, modes) % (2 * count + 2)
    return np.pi / (count + 1) * rank


def split_np(table):
    high = table.astype(np.float32).astype(BF16)
    low = (table - high.astype(np.float64)).astype(np.float32).astype(BF16)
    return high, low


def left_table(count):
    gain = (2.0 / (count + 1)) ** 0.5
    table = np.sin(angles(np.arange(1, count // 2 + 1), np.arange(1, count + 1), count)) * gain
    return split_np(table)


def stacked(high, low):
    return np.block([[high, high], [low, np.zeros_like(low)]])


def long_tables(count):
    modes = np.arange(1, count // 2 + 1)
    gain = (2.0 / (count + 1)) ** 0.5
    coarse = angles(np.arange(0, count, FINE), modes, count)
    step = angles(np.arange(1, FINE + 1), modes, count)
    parts = (np.sin(coarse) * gain, np.cos(coarse) * gain, np.sin(step), np.cos(step))
    return jnp.asarray(np.concatenate(parts).astype(np.float32))


def split(values):
    high = values.astype(BF16)
    return high, (values - high.astype(F32)).astype(BF16)


def dot(a, b):
    return jnp.dot(a, b, preferred_element_type=F32)


def loop(count, body):
    if count == 1:
        body(0)
    else:
        lax.fori_loop(0, count, lambda i, c: (body(i), c)[1], 0)


def kernel(
    north, deep, each,
    src, tx_in, ty_in, *rest,
):
    waves_in, sx_in, sy_in, sz_in, out = rest[:5]
    tx, ty, waves, symbol_z = rest[5:9]
    field, turned, send1, recv1, send2, recv2, send3, recv3, t_high, t_low, left_all, left = rest[9:21]
    symbol_x, symbol_y, fs, ins, sent, r1, r2, r3 = rest[21:]

    me_n, me_d = lax.axis_index("north"), lax.axis_index("deep")
    nx, ny_part, nz_part = src.shape
    halves = ny_part // SUB
    kept_z = t_high.shape[1]
    kept_y = ny_part * north // 2
    share_y = kept_y // deep
    half = north // 2
    pairs = deep // 2
    my_pair = me_d // 2
    far = jnp.where(me_n < half, half, 0)
    bases = (far, half - far)
    last = each - 1
    parts = kept_z // TILE

    loads = {}
    small = []

    def fetch(what, to):
        copy = pltpu.make_async_copy(what, to, ins.at[len(small)])
        copy.start()
        small.append(copy)

    fetch(tx_in, tx)
    for i, (h, c) in enumerate((h, c) for h in range(halves) for c in range(0, nz_part, TILE)):
        loads[h, c] = pltpu.make_async_copy(
            src.at[:, h * SUB : (h + 1) * SUB, c : c + TILE], field.at[h, :, :, c : c + TILE], fs.at[i]
        )
        loads[h, c].start()
    for what, to in zip(
        (waves_in, ty_in, sx_in, sy_in, sz_in),
        (waves, ty, symbol_x, symbol_y, symbol_z),
    ):
        fetch(what, to)

    barrier = pltpu.get_barrier_semaphore()
    for r in range(1, deep):
        pl.semaphore_signal(barrier, inc=1, device_id={"deep": lax.rem(me_d + r, deep)})
    for r in range(1, north):
        pl.semaphore_signal(barrier, inc=1, device_id={"north": lax.rem(me_n + r, north)})

    def x_product(h, c):
        loads[h, c].wait()
        block = min(nx, 128)

        def turn(g):
            for k in range(0, block, 16):
                at = pl.multiple_of(g * block + k, 16)
                high, low = split(jnp.swapaxes(field[h, pl.ds(at, 16), :, c : c + TILE], 0, 1))
                turned[:, pl.ds(at, 16), :] = high
                turned[:, pl.ds(pl.multiple_of(nx + at, 16), 16), :] = low

        loop(nx // block, turn)
        rows = tx.shape[1] // 2
        group = rows // north

        def modes_of(g):
            modes = []
            for y in range(SUB):
                both = dot(tx[g], turned[y])
                modes.append(both[:rows] + both[rows:])
            for k in range(group):
                block = jnp.stack([m[k * north : (k + 1) * north] for m in modes])
                ed = g * group + k
                send1[ed // deep, lax.rem(ed, deep), h, :, :, c : c + TILE] = jnp.swapaxes(block, 0, 1)

        loop(tx.shape[0], modes_of)

    chunks = []
    for f in range(2):
        for e in range(each):
            for h in range(halves):
                cut = half // 2 if not chunks and half % 2 == 0 else half
                chunks += [(f, e, h, i, cut) for i in range(0, half, cut)]

    def copy1(q, r):
        f, e, h, i, count = chunks[q]
        at = pl.ds(bases[f] + i, count)
        to = lax.bitwise_xor(me_d, r)
        key = 2 * each * halves + 1 + f * each + e if r == 1 else q
        return pltpu.make_async_remote_copy(
            src_ref=send1.at[e, to, h, at],
            dst_ref=recv1.at[e, me_d, h, at],
            send_sem=sent.at[0],
            recv_sem=r1.at[key],
            device_id={"deep": to},
        )

    def send_modes(h_done):
        for q, chunk in enumerate(chunks):
            if (q < half // chunks[0][4]) == (h_done == 0):
                for r in (*range(2, deep), 1):
                    copy1(q, r).start()

    for h in range(halves):
        for c in range(0, nz_part, TILE):
            if (h, c) == (0, 0):
                small[0].wait()
            x_product(h, c)
        if h == 0:
            pl.semaphore_wait(barrier, deep + north - 2)
            send_modes(0)
    send_modes(1)

    for copy in small[1:]:
        copy.wait()

    coarse = waves.shape[0] // 2 - FINE

    def table_tile(c):
        cols = slice(c, c + TILE)
        cos_b = waves[2 * coarse + FINE :, cols]
        sin_b = waves[2 * coarse : 2 * coarse + FINE, cols]

        def table_step(g):
            for k in range(4):
                a = g * 4 + k
                table = waves[pl.ds(a, 1), cols] * cos_b + waves[pl.ds(coarse + a, 1), cols] * sin_b
                high, low = split(table)
                at = pl.multiple_of(a * FINE, FINE)
                t_high[pl.ds(at, FINE), cols] = high
                t_low[pl.ds(at, FINE), cols] = low

        loop(coarse // 4, table_step)

    tiles = range(0, kept_z, TILE)

    def z_tile(lhs, count, pair, c):
        at = pl.ds(pl.multiple_of(pair * 2 * nz_part, 2 * nz_part), 2 * nz_part)
        both = dot(lhs[: 2 * count], t_high[at, c : c + TILE])
        return both[:count] + both[count:] + dot(lhs[:count], t_low[at, c : c + TILE])

    def near_left(f, e):
        at = pl.ds(bases[f], half)
        block = recv1.at[e, lax.bitwise_xor(me_d, 1), :, at]
        pltpu.make_async_copy(block, block, r1.at[2 * each * halves + 1 + f * each + e]).wait()
        count = halves * half * SUB
        for owner, block in ((me_d, send1), (lax.bitwise_xor(me_d, 1), recv1)):
            high, low = split(block[e, owner, :, at].reshape(count, nz_part))
            cols = pl.ds(pl.multiple_of(lax.rem(owner, 2) * nz_part, nz_part), nz_part)
            left_all[:count, cols] = high
            left_all[count:, cols] = low

    def near_tile(f, e, c):
        value = z_tile(left_all, halves * half * SUB, my_pair, c).reshape(halves, half, SUB, TILE)
        for h in range(halves):
            send2[e, pl.ds(bases[f], half), h * SUB : (h + 1) * SUB, c : c + TILE] = value[h]

    def far_left(q, pair):
        f, e, h, i, count = chunks[q]
        at, rows = pl.ds(bases[f] + i, count), count * SUB
        block = recv1.at[e, pl.ds(pair * 2, 2), h, at]
        pltpu.make_async_copy(block, block, r1.at[q]).wait()
        for k in range(2):
            high, low = split(recv1[e, pair * 2 + k, h, at].reshape(rows, nz_part))
            left[:rows, k * nz_part : (k + 1) * nz_part] = high
            left[rows : 2 * rows, k * nz_part : (k + 1) * nz_part] = low

    def far_tile(q, pair, c):
        f, e, h, i, count = chunks[q]
        value = z_tile(left, count * SUB, pair, c).reshape(count, SUB, TILE)
        send2[e, pl.ds(bases[f] + i, count), h * SUB : (h + 1) * SUB, c : c + TILE] += value

    def inverse_roots():
        row = lax.broadcasted_iota(jnp.int32, (share_y, TILE), 0)
        part_y = jnp.zeros((share_y, TILE), F32)
        for j in range(share_y):
            part_y = jnp.where(row == j, symbol_y[me_d * share_y + j], part_y)
        for d in range(deep):
            for e in range(each):
                part_x = symbol_x[me_n * deep * each + d * each + e]
                for c in range(0, kept_z, TILE):
                    out[d, e, :, c : c + TILE] = lax.rsqrt(part_x + part_y + symbol_z[:, c : c + TILE])

    def copy2(e, rows, cols, n):
        return pltpu.make_async_remote_copy(
            src_ref=send2.at[e, n, rows, cols],
            dst_ref=recv2.at[e, me_n, rows, cols],
            send_sem=sent.at[1],
            recv_sem=r2.at[e + (cols.start // TILE if e == last else 0)],
            device_id={"north": n},
        )

    def every(count, body):
        if count <= 8:
            for i in range(count):
                body(i)
        else:
            loop(count, body)

    def send_north(f, e, rows, cols, n):
        if f == 0:
            copy2(e, rows, cols, n).start()
        else:
            pl.when(n != me_n)(lambda: copy2(e, rows, cols, n).start())

    def send_slice(f, u, n):
        send_north(f, last, slice(0, ny_part), slice(u * TILE, (u + 1) * TILE), bases[f] + n)

    def copy3(e, p, r):
        to = lax.bitwise_xor(me_d, r)
        cols = slice(p * TILE, (p + 1) * TILE) if e == last else slice(None)
        return pltpu.make_async_remote_copy(
            src_ref=send3.at[e, to, :, cols],
            dst_ref=recv3.at[me_d, e, :, cols],
            send_sem=sent.at[2],
            recv_sem=r3.at[e + p],
            device_id={"deep": to},
        )

    def y_stage(e, p):
        cols = slice(p * TILE, (p + 1) * TILE) if e == last else slice(None)
        block = recv2.at[e, pl.ds(0, north - 1), :, cols]
        pltpu.make_async_copy(block, block, r2.at[e + p]).wait()
        for c in range(0, kept_z, TILE) if e < last else (p * TILE,):
            values = recv2[e, :, :, c : c + TILE].reshape(ny_part * north, TILE)
            both = dot(ty[...], jnp.concatenate(split(values), axis=0))
            modes = both[:kept_y] + both[kept_y:]
            send3[e, :, :, c : c + TILE] = modes.reshape(deep, share_y, TILE)
        for r in (*range(2, deep), 1):
            copy3(e, p, r).start()

    far_chunks = sum(chunk[0] == 0 for chunk in chunks)
    rivals = [lax.rem(my_pair + k, pairs) for k in range(1, pairs)]
    whole = slice(0, kept_z)
    for q, (f, e, h, i, count) in enumerate(chunks):
        lines = slice(h * SUB, (h + 1) * SUB)
        if q == 0:
            for c0 in range(0, kept_z, WIDE):
                wide = range(c0, c0 + WIDE, TILE)
                for c in wide:
                    table_tile(c)
                if c0 == 0:
                    near_left(f, e)
                for c in wide:
                    near_tile(f, e, c)
                if len(rivals) == 1:
                    if c0 == 0:
                        far_left(q, rivals[0])
                    for c in wide:
                        far_tile(q, rivals[0], c)
                    if e < last:
                        every(count, lambda k: send_north(f, e, lines, slice(c0, c0 + WIDE), bases[f] + i + k))
            inverse_roots()
            if len(rivals) == 1:
                continue
        elif h == 0 and i == 0:
            near_left(f, e)
            for c in tiles:
                near_tile(f, e, c)
        for pair in rivals:
            far_left(q, pair)
            for c in tiles:
                far_tile(q, pair, c)
        if e < last:
            every(count, lambda k: send_north(f, e, lines, whole, bases[f] + i + k))
        elif h == halves - 1:
            for u in range(parts) if f else range(2):
                every(half, lambda n: send_slice(f, u, n))
        if f and each > 1:
            u = q - far_chunks + 2
            if u < parts:
                every(half - 1, lambda n: send_slice(0, u, n + 1))
        if q + 1 >= far_chunks and each > 1:
            u = q - far_chunks + 3
            if u < parts:
                send_slice(0, u, 0)

    for e in range(each):
        recv2[e, me_n] = send2[e, me_n]
    for e in range(each):
        for p in range(parts if e == last else 1):
            y_stage(e, p)

    for e in range(each):
        out[me_d, e] = out[me_d, e] * send3[e, me_d]
        for p in range(parts if e == last else 1):
            cols = slice(p * TILE, (p + 1) * TILE) if e == last else slice(None)
            block = recv3.at[pl.ds(0, deep - 1), e, :, cols]
            pltpu.make_async_copy(block, block, r3.at[e + p]).wait()
            for r in range(1, deep):
                owner = lax.bitwise_xor(me_d, r)
                out[owner, e, :, cols] = out[owner, e, :, cols] * recv3[owner, e, :, cols]
    for i, block in enumerate((
        send1.at[:, pl.ds(0, deep - 1)],
        send2.at[:, pl.ds(0, north - 1)],
        send3.at[:, pl.ds(0, deep - 1)],
    )):
        pltpu.make_async_copy(block, block, sent.at[i]).wait()


def on_device(source, symbol_x, symbol_y, symbol_z):
    north, deep = lax.axis_size("north"), lax.axis_size("deep")
    nx, ny_part, nz_part = source.shape
    each, halves = nx // 2 // north // deep, ny_part // SUB
    ny, nz = ny_part * north, nz_part * deep
    kept_z, share_y = nz // 2, ny // 2 // deep
    order = np.arange(nx // 2).reshape(north, deep, each).transpose(2, 1, 0).reshape(-1)
    x_high, x_low = left_table(nx)
    rows = max(ROWS, north)
    tx = jnp.asarray(np.stack([stacked(x_high[o], x_low[o]) for o in order.reshape(-1, rows)]))
    ty = jnp.asarray(stacked(*left_table(ny)))
    waves = long_tables(nz)
    remote = pl.BlockSpec(memory_space=pltpu.HBM)
    rows = SUB * north
    chunks = 2 * each * halves + 1
    operands = (source, tx, ty, waves, symbol_x, symbol_y, symbol_z[None, :])
    buffers = [
        *((t.shape, t.dtype) for t in (tx, ty, waves)),
        ((1, nz), F32),
        ((halves, nx, SUB, nz_part), F32),
        ((SUB, 2 * nx, TILE), BF16),
        ((each, deep, halves, north, SUB, nz_part), F32),
        ((each, deep, halves, north, SUB, nz_part), F32),
        ((each, north, ny_part, kept_z), F32),
        ((each, north, ny_part, kept_z), F32),
        ((each, deep, share_y, kept_z), F32),
        ((deep, each, share_y, kept_z), F32),
        ((nz, kept_z), BF16),
        ((nz, kept_z), BF16),
        ((halves * rows, 2 * nz_part), BF16),
        ((rows, 2 * nz_part), BF16),
    ]
    used = sum(int(np.prod(shape)) * jnp.dtype(kind).itemsize for shape, kind in buffers)
    limit = MOST - SPARE if used < MOST - 2 * SPARE else MOST
    v = pl.pallas_call(
        functools.partial(kernel, north, deep, each),
        out_shape=jax.ShapeDtypeStruct((deep, each, share_y, kept_z), F32),
        in_specs=[remote] * len(operands),
        out_specs=pl.BlockSpec(memory_space=pltpu.VMEM),
        scratch_shapes=[pltpu.VMEM(shape, kind) for shape, kind in buffers]
        + [
            pltpu.SMEM(symbol_x.shape, F32),
            pltpu.SMEM(symbol_y.shape, F32),
            pltpu.SemaphoreType.DMA((halves * nz_part // TILE,)),
            pltpu.SemaphoreType.DMA((len(operands) - 1,)),
        ]
        + [
            pltpu.SemaphoreType.DMA((count,))
            for count in (3, chunks + 2 * each, each + kept_z // TILE, each + kept_z // TILE)
        ],
        compiler_params=pltpu.CompilerParams(
            collective_id=0, has_side_effects=True, vmem_limit_bytes=limit
        ),
    )(*(pltpu.with_memory_space_constraint(operand, pltpu.HBM) for operand in operands))
    return v.reshape(deep * each, share_y, kept_z)


def solution(mesh):
    in_specs = (P(None, "north", "deep"), P(), P(), P())
    out_specs = P("north", "deep", None)
    return jax.shard_map(
        on_device, mesh=mesh, in_specs=in_specs, out_specs=out_specs, check_vma=False
    )
```

```python
import functools

import jax
import jax.numpy as jnp
import numpy as np
from jax import lax
from jax.experimental import pallas as pl
from jax.experimental.pallas import tpu as pltpu
from jax.sharding import PartitionSpec as P

F32, BF16 = jnp.float32, jnp.bfloat16
FINE = 32
TILE = 256
WIDE = 512
SUB = 8
ROWS = 64
MOST = 67043328
SPARE = 14 << 20


def angles(rows, modes, count):
    rank = np.outer(rows, modes) % (2 * count + 2)
    return np.pi / (count + 1) * rank


def split_np(table):
    high = table.astype(np.float32).astype(BF16)
    low = (table - high.astype(np.float64)).astype(np.float32).astype(BF16)
    return high, low


def left_table(count):
    gain = (2.0 / (count + 1)) ** 0.5
    table = np.sin(angles(np.arange(1, count // 2 + 1), np.arange(1, count + 1), count)) * gain
    return split_np(table)


def stacked(high, low):
    return np.block([[high, high], [low, np.zeros_like(low)]])


def long_tables(count):
    modes = np.arange(1, count // 2 + 1)
    gain = (2.0 / (count + 1)) ** 0.5
    coarse = angles(np.arange(0, count, FINE), modes, count)
    step = angles(np.arange(1, FINE + 1), modes, count)
    parts = (np.sin(coarse) * gain, np.cos(coarse) * gain, np.sin(step), np.cos(step))
    return jnp.asarray(np.concatenate(parts).astype(np.float32))


def split(values):
    high = values.astype(BF16)
    return high, (values - high.astype(F32)).astype(BF16)


def dot(a, b):
    return jnp.dot(a, b, preferred_element_type=F32)


def loop(count, body):
    if count == 1:
        body(0)
    else:
        lax.fori_loop(0, count, lambda i, c: (body(i), c)[1], 0)


def kernel(
    north, deep, each,
    src, tx_in, ty_in, *rest,
):
    waves_in, sx_in, sy_in, sz_in, out = rest[:5]
    tx, ty, waves, symbol_z = rest[5:9]
    field, turned, send1, recv1, send2, recv2, send3, recv3, t_high, t_low, left_all, left = rest[9:21]
    symbol_x, symbol_y, fs, ins, sent, r1, r2, r3 = rest[21:]

    me_n, me_d = lax.axis_index("north"), lax.axis_index("deep")
    nx, ny_part, nz_part = src.shape
    halves = ny_part // SUB
    kept_z = t_high.shape[1]
    kept_y = ny_part * north // 2
    share_y = kept_y // deep
    half = north // 2
    pairs = deep // 2
    my_pair = me_d // 2
    far = jnp.where(me_n < half, half, 0)
    bases = (far, half - far)
    last = each - 1
    parts = kept_z // TILE

    loads = {}
    small = []

    def fetch(what, to):
        copy = pltpu.make_async_copy(what, to, ins.at[len(small)])
        copy.start()
        small.append(copy)

    fetch(tx_in, tx)
    for i, (h, c) in enumerate((h, c) for h in range(halves) for c in range(0, nz_part, TILE)):
        loads[h, c] = pltpu.make_async_copy(
            src.at[:, h * SUB : (h + 1) * SUB, c : c + TILE], field.at[h, :, :, c : c + TILE], fs.at[i]
        )
        loads[h, c].start()
    for what, to in zip(
        (waves_in, ty_in, sx_in, sy_in, sz_in),
        (waves, ty, symbol_x, symbol_y, symbol_z),
    ):
        fetch(what, to)

    barrier = pltpu.get_barrier_semaphore()
    for r in range(1, deep):
        pl.semaphore_signal(barrier, inc=1, device_id={"deep": lax.rem(me_d + r, deep)})
    for r in range(1, north):
        pl.semaphore_signal(barrier, inc=1, device_id={"north": lax.rem(me_n + r, north)})

    def x_product(h, c):
        loads[h, c].wait()
        block = min(nx, 128)

        def turn(g):
            for k in range(0, block, 16):
                at = pl.multiple_of(g * block + k, 16)
                high, low = split(jnp.swapaxes(field[h, pl.ds(at, 16), :, c : c + TILE], 0, 1))
                turned[:, pl.ds(at, 16), :] = high
                turned[:, pl.ds(pl.multiple_of(nx + at, 16), 16), :] = low

        loop(nx // block, turn)
        rows = tx.shape[1] // 2
        group = rows // north

        def modes_of(g):
            modes = []
            for y in range(SUB):
                both = dot(tx[g], turned[y])
                modes.append(both[:rows] + both[rows:])
            for k in range(group):
                block = jnp.stack([m[k * north : (k + 1) * north] for m in modes])
                ed = g * group + k
                send1[ed // deep, lax.rem(ed, deep), h, :, :, c : c + TILE] = jnp.swapaxes(block, 0, 1)

        loop(tx.shape[0], modes_of)

    chunks = []
    for f in range(2):
        for e in range(each):
            for h in range(halves):
                cut = half // 2 if not chunks and half % 2 == 0 else half
                chunks += [(f, e, h, i, cut) for i in range(0, half, cut)]

    def copy1(q, r):
        f, e, h, i, count = chunks[q]
        at = pl.ds(bases[f] + i, count)
        to = lax.bitwise_xor(me_d, r)
        key = 2 * each * halves + 1 + f * each + e if r == 1 else q
        return pltpu.make_async_remote_copy(
            src_ref=send1.at[e, to, h, at],
            dst_ref=recv1.at[e, me_d, h, at],
            send_sem=sent.at[0],
            recv_sem=r1.at[key],
            device_id={"deep": to},
        )

    def send_modes(h_done):
        for q, chunk in enumerate(chunks):
            if (q < half // chunks[0][4]) == (h_done == 0):
                for r in (*range(2, deep), 1):
                    copy1(q, r).start()

    for h in range(halves):
        for c in range(0, nz_part, TILE):
            if (h, c) == (0, 0):
                small[0].wait()
            x_product(h, c)
        if h == 0:
            pl.semaphore_wait(barrier, deep + north - 2)
            send_modes(0)
    send_modes(1)

    for copy in small[1:]:
        copy.wait()

    coarse = waves.shape[0] // 2 - FINE

    def table_tile(c):
        cols = slice(c, c + TILE)
        cos_b = waves[2 * coarse + FINE :, cols]
        sin_b = waves[2 * coarse : 2 * coarse + FINE, cols]

        def table_step(g):
            for k in range(4):
                a = g * 4 + k
                table = waves[pl.ds(a, 1), cols] * cos_b + waves[pl.ds(coarse + a, 1), cols] * sin_b
                high, low = split(table)
                at = pl.multiple_of(a * FINE, FINE)
                t_high[pl.ds(at, FINE), cols] = high
                t_low[pl.ds(at, FINE), cols] = low

        loop(coarse // 4, table_step)

    tiles = range(0, kept_z, TILE)

    def z_tile(lhs, count, pair, c):
        at = pl.ds(pl.multiple_of(pair * 2 * nz_part, 2 * nz_part), 2 * nz_part)
        both = dot(lhs[: 2 * count], t_high[at, c : c + TILE])
        return both[:count] + both[count:] + dot(lhs[:count], t_low[at, c : c + TILE])

    def near_left(f, e):
        at = pl.ds(bases[f], half)
        block = recv1.at[e, lax.bitwise_xor(me_d, 1), :, at]
        pltpu.make_async_copy(block, block, r1.at[2 * each * halves + 1 + f * each + e]).wait()
        count = halves * half * SUB
        for owner, block in ((me_d, send1), (lax.bitwise_xor(me_d, 1), recv1)):
            high, low = split(block[e, owner, :, at].reshape(count, nz_part))
            cols = pl.ds(pl.multiple_of(lax.rem(owner, 2) * nz_part, nz_part), nz_part)
            left_all[:count, cols] = high
            left_all[count:, cols] = low

    def near_tile(f, e, c):
        value = z_tile(left_all, halves * half * SUB, my_pair, c).reshape(halves, half, SUB, TILE)
        for h in range(halves):
            send2[e, pl.ds(bases[f], half), h * SUB : (h + 1) * SUB, c : c + TILE] = value[h]

    def far_left(q, pair):
        f, e, h, i, count = chunks[q]
        at, rows = pl.ds(bases[f] + i, count), count * SUB
        block = recv1.at[e, pl.ds(pair * 2, 2), h, at]
        pltpu.make_async_copy(block, block, r1.at[q]).wait()
        for k in range(2):
            high, low = split(recv1[e, pair * 2 + k, h, at].reshape(rows, nz_part))
            left[:rows, k * nz_part : (k + 1) * nz_part] = high
            left[rows : 2 * rows, k * nz_part : (k + 1) * nz_part] = low

    def far_tile(q, pair, c):
        f, e, h, i, count = chunks[q]
        value = z_tile(left, count * SUB, pair, c).reshape(count, SUB, TILE)
        send2[e, pl.ds(bases[f] + i, count), h * SUB : (h + 1) * SUB, c : c + TILE] += value

    def inverse_roots():
        row = lax.broadcasted_iota(jnp.int32, (share_y, TILE), 0)
        part_y = jnp.zeros((share_y, TILE), F32)
        for j in range(share_y):
            part_y = jnp.where(row == j, symbol_y[me_d * share_y + j], part_y)
        for d in range(deep):
            for e in range(each):
                part_x = symbol_x[me_n * deep * each + d * each + e]
                for c in range(0, kept_z, TILE):
                    out[d, e, :, c : c + TILE] = lax.rsqrt(part_x + part_y + symbol_z[:, c : c + TILE])

    def copy2(e, rows, cols, n):
        return pltpu.make_async_remote_copy(
            src_ref=send2.at[e, n, rows, cols],
            dst_ref=recv2.at[e, me_n, rows, cols],
            send_sem=sent.at[1],
            recv_sem=r2.at[e + (cols.start // TILE if e == last else 0)],
            device_id={"north": n},
        )

    def every(count, body):
        if count <= 8:
            for i in range(count):
                body(i)
        else:
            loop(count, body)

    def send_north(f, e, rows, cols, n):
        if f == 0:
            copy2(e, rows, cols, n).start()
        else:
            pl.when(n != me_n)(lambda: copy2(e, rows, cols, n).start())

    def send_slice(f, rows, u, n):
        send_north(f, last, rows, slice(u * TILE, (u + 1) * TILE), bases[f] + n)

    def copy3(e, p, r):
        to = lax.bitwise_xor(me_d, r)
        cols = slice(p * TILE, (p + 1) * TILE) if e == last else slice(None)
        return pltpu.make_async_remote_copy(
            src_ref=send3.at[e, to, :, cols],
            dst_ref=recv3.at[me_d, e, :, cols],
            send_sem=sent.at[2],
            recv_sem=r3.at[e + p],
            device_id={"deep": to},
        )

    def y_stage(e, p):
        cols = slice(p * TILE, (p + 1) * TILE) if e == last else slice(None)
        block = recv2.at[e, pl.ds(0, north - 1), :, cols]
        pltpu.make_async_copy(block, block, r2.at[e + p]).wait()
        for c in range(0, kept_z, TILE) if e < last else (p * TILE,):
            values = recv2[e, :, :, c : c + TILE].reshape(ny_part * north, TILE)
            both = dot(ty[...], jnp.concatenate(split(values), axis=0))
            modes = both[:kept_y] + both[kept_y:]
            send3[e, :, :, c : c + TILE] = modes.reshape(deep, share_y, TILE)
        for r in (*range(2, deep), 1):
            copy3(e, p, r).start()

    far_chunks = sum(chunk[0] == 0 for chunk in chunks)
    rivals = [lax.rem(my_pair + k, pairs) for k in range(1, pairs)]
    whole = slice(0, kept_z)
    for q, (f, e, h, i, count) in enumerate(chunks):
        lines = slice(h * SUB, (h + 1) * SUB)
        if q == 0:
            for c0 in range(0, kept_z, WIDE):
                wide = range(c0, c0 + WIDE, TILE)
                for c in wide:
                    table_tile(c)
                if c0 == 0:
                    near_left(f, e)
                for c in wide:
                    near_tile(f, e, c)
                if len(rivals) == 1:
                    if c0 == 0:
                        far_left(q, rivals[0])
                    for c in wide:
                        far_tile(q, rivals[0], c)
                    if e < last:
                        every(count, lambda k: send_north(f, e, lines, slice(c0, c0 + WIDE), bases[f] + i + k))
            inverse_roots()
            if len(rivals) == 1:
                continue
        elif h == 0 and i == 0:
            near_left(f, e)
            for c in tiles:
                near_tile(f, e, c)
        for pair in rivals:
            far_left(q, pair)
            for c in tiles:
                far_tile(q, pair, c)
        if e < last:
            every(count, lambda k: send_north(f, e, lines, whole, bases[f] + i + k))
        elif f:
            for u in range(parts):
                every(half, lambda n: send_slice(f, lines, u, n))
        if far_chunks - 1 <= q < far_chunks + parts - 1:
            u = q - far_chunks + 1
            for n in range(half):
                v = u + (n < half // 2)
                for v in range(v + 1) if u == 0 else (v,):
                    if v < parts:
                        send_slice(0, slice(0, ny_part), v, n)
        if f and h == halves - 1:
            recv2[e, me_n] = send2[e, me_n]
        if q == len(chunks) - 2:
            for k in range(last):
                y_stage(k, 0)

    for p in range(parts):
        y_stage(last, p)

    for e in range(each):
        out[me_d, e] = out[me_d, e] * send3[e, me_d]
        for p in range(parts if e == last else 1):
            cols = slice(p * TILE, (p + 1) * TILE) if e == last else slice(None)
            block = recv3.at[pl.ds(0, deep - 1), e, :, cols]
            pltpu.make_async_copy(block, block, r3.at[e + p]).wait()
            for r in range(1, deep):
                owner = lax.bitwise_xor(me_d, r)
                out[owner, e, :, cols] = out[owner, e, :, cols] * recv3[owner, e, :, cols]
    for i, block in enumerate((
        send1.at[:, pl.ds(0, deep - 1)],
        send2.at[:, pl.ds(0, north - 1)],
        send3.at[:, pl.ds(0, deep - 1)],
    )):
        pltpu.make_async_copy(block, block, sent.at[i]).wait()


def on_device(source, symbol_x, symbol_y, symbol_z):
    north, deep = lax.axis_size("north"), lax.axis_size("deep")
    nx, ny_part, nz_part = source.shape
    each, halves = nx // 2 // north // deep, ny_part // SUB
    ny, nz = ny_part * north, nz_part * deep
    kept_z, share_y = nz // 2, ny // 2 // deep
    order = np.arange(nx // 2).reshape(north, deep, each).transpose(2, 1, 0).reshape(-1)
    x_high, x_low = left_table(nx)
    rows = max(ROWS, north)
    tx = jnp.asarray(np.stack([stacked(x_high[o], x_low[o]) for o in order.reshape(-1, rows)]))
    ty = jnp.asarray(stacked(*left_table(ny)))
    waves = long_tables(nz)
    remote = pl.BlockSpec(memory_space=pltpu.HBM)
    rows = SUB * north
    chunks = 2 * each * halves + 1
    operands = (source, tx, ty, waves, symbol_x, symbol_y, symbol_z[None, :])
    buffers = [
        *((t.shape, t.dtype) for t in (tx, ty, waves)),
        ((1, nz), F32),
        ((halves, nx, SUB, nz_part), F32),
        ((SUB, 2 * nx, TILE), BF16),
        ((each, deep, halves, north, SUB, nz_part), F32),
        ((each, deep, halves, north, SUB, nz_part), F32),
        ((each, north, ny_part, kept_z), F32),
        ((each, north, ny_part, kept_z), F32),
        ((each, deep, share_y, kept_z), F32),
        ((deep, each, share_y, kept_z), F32),
        ((nz, kept_z), BF16),
        ((nz, kept_z), BF16),
        ((halves * rows, 2 * nz_part), BF16),
        ((rows, 2 * nz_part), BF16),
    ]
    used = sum(int(np.prod(shape)) * jnp.dtype(kind).itemsize for shape, kind in buffers)
    limit = MOST - SPARE if used < MOST - 2 * SPARE else MOST
    v = pl.pallas_call(
        functools.partial(kernel, north, deep, each),
        out_shape=jax.ShapeDtypeStruct((deep, each, share_y, kept_z), F32),
        in_specs=[remote] * len(operands),
        out_specs=pl.BlockSpec(memory_space=pltpu.VMEM),
        scratch_shapes=[pltpu.VMEM(shape, kind) for shape, kind in buffers]
        + [
            pltpu.SMEM(symbol_x.shape, F32),
            pltpu.SMEM(symbol_y.shape, F32),
            pltpu.SemaphoreType.DMA((halves * nz_part // TILE,)),
            pltpu.SemaphoreType.DMA((len(operands) - 1,)),
        ]
        + [
            pltpu.SemaphoreType.DMA((count,))
            for count in (3, chunks + 2 * each, each + kept_z // TILE, each + kept_z // TILE)
        ],
        compiler_params=pltpu.CompilerParams(
            collective_id=0, has_side_effects=True, vmem_limit_bytes=limit
        ),
    )(*(pltpu.with_memory_space_constraint(operand, pltpu.HBM) for operand in operands))
    return v.reshape(deep * each, share_y, kept_z)


def solution(mesh):
    in_specs = (P(None, "north", "deep"), P(), P(), P())
    out_specs = P("north", "deep", None)
    return jax.shard_map(
        on_device, mesh=mesh, in_specs=in_specs, out_specs=out_specs, check_vma=False
    )
```

```python
import functools

import jax
import jax.numpy as jnp
import numpy as np
from jax import lax
from jax.experimental import pallas as pl
from jax.experimental.pallas import tpu as pltpu
from jax.sharding import PartitionSpec as P

F32, BF16 = jnp.float32, jnp.bfloat16
FINE = 32
TILE = 256
WIDE = 512
SUB = 8
ROWS = 64
MOST = 67043328
SPARE = 14 << 20


def angles(rows, modes, count):
    rank = np.outer(rows, modes) % (2 * count + 2)
    return np.pi / (count + 1) * rank


def split_np(table):
    high = table.astype(np.float32).astype(BF16)
    low = (table - high.astype(np.float64)).astype(np.float32).astype(BF16)
    return high, low


def left_table(count):
    gain = (2.0 / (count + 1)) ** 0.5
    table = np.sin(angles(np.arange(1, count // 2 + 1), np.arange(1, count + 1), count)) * gain
    return split_np(table)


def stacked(high, low):
    return np.block([[high, high], [low, np.zeros_like(low)]])


def long_tables(count):
    modes = np.arange(1, count // 2 + 1)
    gain = (2.0 / (count + 1)) ** 0.5
    coarse = angles(np.arange(0, count, FINE), modes, count)
    step = angles(np.arange(1, FINE + 1), modes, count)
    parts = (np.sin(coarse) * gain, np.cos(coarse) * gain, np.sin(step), np.cos(step))
    return jnp.asarray(np.concatenate(parts).astype(np.float32))


def split(values):
    high = values.astype(BF16)
    return high, (values - high.astype(F32)).astype(BF16)


def dot(a, b):
    return jnp.dot(a, b, preferred_element_type=F32)


def loop(count, body):
    if count == 1:
        body(0)
    else:
        lax.fori_loop(0, count, lambda i, c: (body(i), c)[1], 0)


def kernel(
    north, deep, each,
    src, tx_in, ty_in, *rest,
):
    waves_in, sx_in, sy_in, sz_in, out = rest[:5]
    tx, ty, waves, symbol_z = rest[5:9]
    field, turned, send1, recv1, send2, recv2, send3, recv3, t_high, t_low, left_all, left = rest[9:21]
    symbol_x, symbol_y, fs, ins, sent, r1, r2, r3 = rest[21:]

    me_n, me_d = lax.axis_index("north"), lax.axis_index("deep")
    nx, ny_part, nz_part = src.shape
    halves = ny_part // SUB
    kept_z = t_high.shape[1]
    kept_y = ny_part * north // 2
    share_y = kept_y // deep
    half = north // 2
    pairs = deep // 2
    my_pair = me_d // 2
    far = jnp.where(me_n < half, half, 0)
    bases = (far, half - far)
    last = each - 1
    parts = kept_z // TILE

    loads = {}
    small = []

    def fetch(what, to):
        copy = pltpu.make_async_copy(what, to, ins.at[len(small)])
        copy.start()
        small.append(copy)

    fetch(tx_in, tx)
    for i, (h, c) in enumerate((h, c) for h in range(halves) for c in range(0, nz_part, TILE)):
        loads[h, c] = pltpu.make_async_copy(
            src.at[:, h * SUB : (h + 1) * SUB, c : c + TILE], field.at[h, :, :, c : c + TILE], fs.at[i]
        )
        loads[h, c].start()
    for what, to in zip(
        (waves_in, ty_in, sx_in, sy_in, sz_in),
        (waves, ty, symbol_x, symbol_y, symbol_z),
    ):
        fetch(what, to)

    barrier = pltpu.get_barrier_semaphore()
    for r in range(1, deep):
        pl.semaphore_signal(barrier, inc=1, device_id={"deep": lax.rem(me_d + r, deep)})
    for r in range(1, north):
        pl.semaphore_signal(barrier, inc=1, device_id={"north": lax.rem(me_n + r, north)})

    def x_product(h, c):
        loads[h, c].wait()
        block = min(nx, 128)

        def turn(g):
            for k in range(0, block, 16):
                at = pl.multiple_of(g * block + k, 16)
                high, low = split(jnp.swapaxes(field[h, pl.ds(at, 16), :, c : c + TILE], 0, 1))
                turned[:, pl.ds(at, 16), :] = high
                turned[:, pl.ds(pl.multiple_of(nx + at, 16), 16), :] = low

        loop(nx // block, turn)
        rows = tx.shape[1] // 2
        group = rows // north

        def modes_of(g):
            modes = []
            for y in range(SUB):
                both = dot(tx[g], turned[y])
                modes.append(both[:rows] + both[rows:])
            for k in range(group):
                block = jnp.stack([m[k * north : (k + 1) * north] for m in modes])
                ed = g * group + k
                send1[ed // deep, lax.rem(ed, deep), h, :, :, c : c + TILE] = jnp.swapaxes(block, 0, 1)

        loop(tx.shape[0], modes_of)

    chunks = []
    for f in range(2):
        for e in range(each):
            if f and e == last:
                cut = half // 2
                chunks += [(f, e, 0, halves, i, cut) for i in range(0, half, cut)]
                continue
            for h in range(halves):
                cut = half if chunks else half // 2
                chunks += [(f, e, h, 1, i, cut) for i in range(0, half, cut)]

    def copy1(q, r):
        f, e, h, hs, i, count = chunks[q]
        at, h = pl.ds(bases[f] + i, count), pl.ds(h, hs)
        to = lax.bitwise_xor(me_d, r)
        key = len(chunks) + f * each + e if r == 1 else q
        return pltpu.make_async_remote_copy(
            src_ref=send1.at[e, to, h, at],
            dst_ref=recv1.at[e, me_d, h, at],
            send_sem=sent.at[0],
            recv_sem=r1.at[key],
            device_id={"deep": to},
        )

    def send_modes(h_done):
        for q, chunk in enumerate(chunks):
            if (q < 2) == (h_done == 0):
                for r in (*range(2, deep), 1):
                    copy1(q, r).start()

    for h in range(halves):
        for c in range(0, nz_part, TILE):
            if (h, c) == (0, 0):
                small[0].wait()
            x_product(h, c)
        if h == 0:
            pl.semaphore_wait(barrier, deep + north - 2)
            send_modes(0)
    send_modes(1)

    for copy in small[1:]:
        copy.wait()

    coarse = waves.shape[0] // 2 - FINE

    def table_tile(c):
        cols = slice(c, c + TILE)
        cos_b = waves[2 * coarse + FINE :, cols]
        sin_b = waves[2 * coarse : 2 * coarse + FINE, cols]

        def table_step(g):
            for k in range(4):
                a = g * 4 + k
                table = waves[pl.ds(a, 1), cols] * cos_b + waves[pl.ds(coarse + a, 1), cols] * sin_b
                high, low = split(table)
                at = pl.multiple_of(a * FINE, FINE)
                t_high[pl.ds(at, FINE), cols] = high
                t_low[pl.ds(at, FINE), cols] = low

        loop(coarse // 4, table_step)

    tiles = range(0, kept_z, TILE)

    def z_tile(lhs, count, pair, c):
        at = pl.ds(pl.multiple_of(pair * 2 * nz_part, 2 * nz_part), 2 * nz_part)
        both = dot(lhs[: 2 * count], t_high[at, c : c + TILE])
        return both[:count] + both[count:] + dot(lhs[:count], t_low[at, c : c + TILE])

    def near_left(f, e):
        at = pl.ds(bases[f], half)
        block = recv1.at[e, lax.bitwise_xor(me_d, 1), :, at]
        pltpu.make_async_copy(block, block, r1.at[len(chunks) + f * each + e]).wait()
        count = halves * half * SUB
        for owner, block in ((me_d, send1), (lax.bitwise_xor(me_d, 1), recv1)):
            high, low = split(block[e, owner, :, at].reshape(count, nz_part))
            cols = pl.ds(pl.multiple_of(lax.rem(owner, 2) * nz_part, nz_part), nz_part)
            left_all[:count, cols] = high
            left_all[count:, cols] = low

    def near_tile(f, e, c):
        value = z_tile(left_all, halves * half * SUB, my_pair, c).reshape(halves, half, SUB, TILE)
        for h in range(halves):
            send2[e, pl.ds(bases[f], half), h * SUB : (h + 1) * SUB, c : c + TILE] = value[h]

    def far_left(q, pair):
        f, e, h, hs, i, count = chunks[q]
        at, rows, h = pl.ds(bases[f] + i, count), hs * count * SUB, pl.ds(h, hs)
        block = recv1.at[e, pl.ds(pair * 2, 2), h, at]
        pltpu.make_async_copy(block, block, r1.at[q]).wait()
        for k in range(2):
            high, low = split(recv1[e, pair * 2 + k, h, at].reshape(rows, nz_part))
            left[:rows, k * nz_part : (k + 1) * nz_part] = high
            left[rows : 2 * rows, k * nz_part : (k + 1) * nz_part] = low

    def far_tile(q, pair, c):
        f, e, h, hs, i, count = chunks[q]
        value = z_tile(left, hs * count * SUB, pair, c).reshape(hs, count, SUB, TILE)
        for k in range(hs):
            rows = slice((h + k) * SUB, (h + k + 1) * SUB)
            send2[e, pl.ds(bases[f] + i, count), rows, c : c + TILE] += value[k]

    def inverse_roots():
        row = lax.broadcasted_iota(jnp.int32, (share_y, TILE), 0)
        part_y = jnp.zeros((share_y, TILE), F32)
        for j in range(share_y):
            part_y = jnp.where(row == j, symbol_y[me_d * share_y + j], part_y)
        for d in range(deep):
            for e in range(each):
                part_x = symbol_x[me_n * deep * each + d * each + e]
                for c in range(0, kept_z, TILE):
                    out[d, e, :, c : c + TILE] = lax.rsqrt(part_x + part_y + symbol_z[:, c : c + TILE])

    def copy2(e, rows, cols, n):
        return pltpu.make_async_remote_copy(
            src_ref=send2.at[e, n, rows, cols],
            dst_ref=recv2.at[e, me_n, rows, cols],
            send_sem=sent.at[1],
            recv_sem=r2.at[e + (cols.start // TILE if e == last else 0)],
            device_id={"north": n},
        )

    def every(count, body):
        if count <= 8:
            for i in range(count):
                body(i)
        else:
            loop(count, body)

    def send_north(f, e, rows, cols, n):
        if f == 0:
            copy2(e, rows, cols, n).start()
        else:
            pl.when(n != me_n)(lambda: copy2(e, rows, cols, n).start())

    def send_slice(f, rows, u, n):
        send_north(f, last, rows, slice(u * TILE, (u + 1) * TILE), bases[f] + n)

    def copy3(e, p, r):
        to = lax.bitwise_xor(me_d, r)
        cols = slice(p * TILE, (p + 1) * TILE) if e == last else slice(None)
        return pltpu.make_async_remote_copy(
            src_ref=send3.at[e, to, :, cols],
            dst_ref=recv3.at[me_d, e, :, cols],
            send_sem=sent.at[2],
            recv_sem=r3.at[e + p],
            device_id={"deep": to},
        )

    def y_stage(e, p):
        cols = slice(p * TILE, (p + 1) * TILE) if e == last else slice(None)
        block = recv2.at[e, pl.ds(0, north - 1), :, cols]
        pltpu.make_async_copy(block, block, r2.at[e + p]).wait()
        for c in range(0, kept_z, TILE) if e < last else (p * TILE,):
            values = recv2[e, :, :, c : c + TILE].reshape(ny_part * north, TILE)
            both = dot(ty[...], jnp.concatenate(split(values), axis=0))
            modes = both[:kept_y] + both[kept_y:]
            send3[e, :, :, c : c + TILE] = modes.reshape(deep, share_y, TILE)
        for r in (*range(2, deep), 1):
            copy3(e, p, r).start()

    far_chunks = sum(chunk[0] == 0 for chunk in chunks)
    rivals = [lax.rem(my_pair + k, pairs) for k in range(1, pairs)]
    whole = slice(0, kept_z)
    for q, (f, e, h, hs, i, count) in enumerate(chunks):
        lines = slice(h * SUB, (h + hs) * SUB)
        if q == 0:
            for c0 in range(0, kept_z, WIDE):
                wide = range(c0, c0 + WIDE, TILE)
                for c in wide:
                    table_tile(c)
                if c0 == 0:
                    near_left(f, e)
                for c in wide:
                    near_tile(f, e, c)
                if len(rivals) == 1:
                    if c0 == 0:
                        far_left(q, rivals[0])
                    for c in wide:
                        far_tile(q, rivals[0], c)
                    if e < last:
                        every(count, lambda k: send_north(f, e, lines, slice(c0, c0 + WIDE), bases[f] + i + k))
            inverse_roots()
            if len(rivals) == 1:
                continue
        elif h == 0 and i == 0:
            near_left(f, e)
            for c in tiles:
                near_tile(f, e, c)
        for pair in rivals:
            far_left(q, pair)
            for c in tiles:
                far_tile(q, pair, c)
        if e < last:
            every(count, lambda k: send_north(f, e, lines, whole, bases[f] + i + k))
        elif f:
            for u in range(parts):
                every(count, lambda n: send_slice(f, lines, u, i + n))
        u = q - far_chunks + 1
        if 0 <= u < parts - 1:
            every(half, lambda n: send_slice(0, slice(0, ny_part), u, n))
        elif parts - 1 <= u <= parts:
            every(half // 2, lambda n: send_slice(0, slice(0, ny_part), parts - 1, n + (u == parts) * (half // 2)))
        if f and h + hs == halves and i + count == half:
            recv2[e, me_n] = send2[e, me_n]
        if q == len(chunks) - 2:
            for k in range(last):
                y_stage(k, 0)

    for p in range(parts):
        y_stage(last, p)

    for e in range(each):
        out[me_d, e] = out[me_d, e] * send3[e, me_d]
        for p in range(parts if e == last else 1):
            cols = slice(p * TILE, (p + 1) * TILE) if e == last else slice(None)
            block = recv3.at[pl.ds(0, deep - 1), e, :, cols]
            pltpu.make_async_copy(block, block, r3.at[e + p]).wait()
            for r in range(1, deep):
                owner = lax.bitwise_xor(me_d, r)
                out[owner, e, :, cols] = out[owner, e, :, cols] * recv3[owner, e, :, cols]
    for i, block in enumerate((
        send1.at[:, pl.ds(0, deep - 1)],
        send2.at[:, pl.ds(0, north - 1)],
        send3.at[:, pl.ds(0, deep - 1)],
    )):
        pltpu.make_async_copy(block, block, sent.at[i]).wait()


def on_device(source, symbol_x, symbol_y, symbol_z):
    north, deep = lax.axis_size("north"), lax.axis_size("deep")
    nx, ny_part, nz_part = source.shape
    each, halves = nx // 2 // north // deep, ny_part // SUB
    ny, nz = ny_part * north, nz_part * deep
    kept_z, share_y = nz // 2, ny // 2 // deep
    order = np.arange(nx // 2).reshape(north, deep, each).transpose(2, 1, 0).reshape(-1)
    x_high, x_low = left_table(nx)
    rows = max(ROWS, north)
    tx = jnp.asarray(np.stack([stacked(x_high[o], x_low[o]) for o in order.reshape(-1, rows)]))
    ty = jnp.asarray(stacked(*left_table(ny)))
    waves = long_tables(nz)
    remote = pl.BlockSpec(memory_space=pltpu.HBM)
    rows = SUB * north
    chunks = 2 * each * halves + 3 - halves
    operands = (source, tx, ty, waves, symbol_x, symbol_y, symbol_z[None, :])
    buffers = [
        *((t.shape, t.dtype) for t in (tx, ty, waves)),
        ((1, nz), F32),
        ((halves, nx, SUB, nz_part), F32),
        ((SUB, 2 * nx, TILE), BF16),
        ((each, deep, halves, north, SUB, nz_part), F32),
        ((each, deep, halves, north, SUB, nz_part), F32),
        ((each, north, ny_part, kept_z), F32),
        ((each, north, ny_part, kept_z), F32),
        ((each, deep, share_y, kept_z), F32),
        ((deep, each, share_y, kept_z), F32),
        ((nz, kept_z), BF16),
        ((nz, kept_z), BF16),
        ((halves * rows, 2 * nz_part), BF16),
        ((rows, 2 * nz_part), BF16),
    ]
    used = sum(int(np.prod(shape)) * jnp.dtype(kind).itemsize for shape, kind in buffers)
    limit = MOST - SPARE if used < MOST - 2 * SPARE else MOST
    v = pl.pallas_call(
        functools.partial(kernel, north, deep, each),
        out_shape=jax.ShapeDtypeStruct((deep, each, share_y, kept_z), F32),
        in_specs=[remote] * len(operands),
        out_specs=pl.BlockSpec(memory_space=pltpu.VMEM),
        scratch_shapes=[pltpu.VMEM(shape, kind) for shape, kind in buffers]
        + [
            pltpu.SMEM(symbol_x.shape, F32),
            pltpu.SMEM(symbol_y.shape, F32),
            pltpu.SemaphoreType.DMA((halves * nz_part // TILE,)),
            pltpu.SemaphoreType.DMA((len(operands) - 1,)),
        ]
        + [
            pltpu.SemaphoreType.DMA((count,))
            for count in (3, chunks + 2 * each, each + kept_z // TILE, each + kept_z // TILE)
        ],
        compiler_params=pltpu.CompilerParams(
            collective_id=0, has_side_effects=True, vmem_limit_bytes=limit
        ),
    )(*(pltpu.with_memory_space_constraint(operand, pltpu.HBM) for operand in operands))
    return v.reshape(deep * each, share_y, kept_z)


def solution(mesh):
    in_specs = (P(None, "north", "deep"), P(), P(), P())
    out_specs = P("north", "deep", None)
    return jax.shard_map(
        on_device, mesh=mesh, in_specs=in_specs, out_specs=out_specs, check_vma=False
    )
```

```python
import functools

import jax
import jax.numpy as jnp
import numpy as np
from jax import lax
from jax.experimental import pallas as pl
from jax.experimental.pallas import tpu as pltpu
from jax.sharding import PartitionSpec as P

F32, BF16 = jnp.float32, jnp.bfloat16
FINE = 32
TILE = 256
WIDE = 512
SUB = 8
ROWS = 64
MOST = 67043328
SPARE = 14 << 20


def angles(rows, modes, count):
    rank = np.outer(rows, modes) % (2 * count + 2)
    return np.pi / (count + 1) * rank


def split_np(table):
    high = table.astype(np.float32).astype(BF16)
    low = (table - high.astype(np.float64)).astype(np.float32).astype(BF16)
    return high, low


def left_table(count):
    gain = (2.0 / (count + 1)) ** 0.5
    table = np.sin(angles(np.arange(1, count // 2 + 1), np.arange(1, count + 1), count)) * gain
    return split_np(table)


def stacked(high, low):
    return np.block([[high, high], [low, np.zeros_like(low)]])


def long_tables(count):
    modes = np.arange(1, count // 2 + 1)
    gain = (2.0 / (count + 1)) ** 0.5
    coarse = angles(np.arange(0, count, FINE), modes, count)
    step = angles(np.arange(1, FINE + 1), modes, count)
    parts = (np.sin(coarse) * gain, np.cos(coarse) * gain, np.sin(step), np.cos(step))
    return jnp.asarray(np.concatenate(parts).astype(np.float32))


def split(values):
    high = values.astype(BF16)
    return high, (values - high.astype(F32)).astype(BF16)


def dot(a, b):
    return jnp.dot(a, b, preferred_element_type=F32)


def loop(count, body):
    if count == 1:
        body(0)
    else:
        lax.fori_loop(0, count, lambda i, c: (body(i), c)[1], 0)


def kernel(
    north, deep, each,
    src, tx_in, ty_in, *rest,
):
    waves_in, sx_in, sy_in, sz_in, out = rest[:5]
    tx, ty, waves, symbol_z = rest[5:9]
    field, turned, send1, recv1, send2, recv2, send3, recv3, t_high, t_low, left_all, left = rest[9:21]
    symbol_x, symbol_y, fs, ins, sent, r1, r2, r3 = rest[21:]

    me_n, me_d = lax.axis_index("north"), lax.axis_index("deep")
    nx, ny_part, nz_part = src.shape
    halves = ny_part // SUB
    kept_z = t_high.shape[1]
    kept_y = ny_part * north // 2
    share_y = kept_y // deep
    half = north // 2
    pairs = deep // 2
    my_pair = me_d // 2
    far = jnp.where(me_n < half, half, 0)
    bases = (far, half - far)
    last = each - 1
    parts = kept_z // TILE

    loads = {}
    small = []

    def fetch(what, to):
        copy = pltpu.make_async_copy(what, to, ins.at[len(small)])
        copy.start()
        small.append(copy)

    fetch(tx_in, tx)
    for i, (h, c) in enumerate((h, c) for h in range(halves) for c in range(0, nz_part, TILE)):
        loads[h, c] = pltpu.make_async_copy(
            src.at[:, h * SUB : (h + 1) * SUB, c : c + TILE], field.at[h, :, :, c : c + TILE], fs.at[i]
        )
        loads[h, c].start()
    for what, to in zip(
        (waves_in, ty_in, sx_in, sy_in, sz_in),
        (waves, ty, symbol_x, symbol_y, symbol_z),
    ):
        fetch(what, to)

    barrier = pltpu.get_barrier_semaphore()
    for r in range(1, deep):
        pl.semaphore_signal(barrier, inc=1, device_id={"deep": lax.rem(me_d + r, deep)})
    for r in range(1, north):
        pl.semaphore_signal(barrier, inc=1, device_id={"north": lax.rem(me_n + r, north)})

    def x_product(h, c):
        loads[h, c].wait()
        block = min(nx, 128)

        def turn(g):
            for k in range(0, block, 16):
                at = pl.multiple_of(g * block + k, 16)
                high, low = split(jnp.swapaxes(field[h, pl.ds(at, 16), :, c : c + TILE], 0, 1))
                turned[:, pl.ds(at, 16), :] = high
                turned[:, pl.ds(pl.multiple_of(nx + at, 16), 16), :] = low

        loop(nx // block, turn)
        rows = tx.shape[1] // 2
        group = rows // north

        def modes_of(g):
            modes = []
            for y in range(SUB):
                both = dot(tx[g], turned[y])
                modes.append(both[:rows] + both[rows:])
            for k in range(group):
                block = jnp.stack([m[k * north : (k + 1) * north] for m in modes])
                ed = g * group + k
                send1[ed // deep, lax.rem(ed, deep), h, :, :, c : c + TILE] = jnp.swapaxes(block, 0, 1)

        loop(tx.shape[0], modes_of)

    chunks = []
    for e in range(each):
        for h in range(halves):
            cut = half if chunks else half // 2
            chunks += [(0, e, h, 1, i, cut) for i in range(0, half, cut)]
    for e in range(each):
        chunks += [(1, e, 0, halves, i, half // 2) for i in range(0, half, half // 2)]

    def start_of(q):
        f, e, _, _, i, count = chunks[q]
        if f and e < last:
            i = jnp.where(me_n < half, i, half - count - i)
        return bases[f] + i

    def copy1(q, r):
        f, e, h, hs, i, count = chunks[q]
        at, h = pl.ds(start_of(q), count), pl.ds(h, hs)
        to = lax.bitwise_xor(me_d, r)
        key = len(chunks) + f * each + e if r == 1 else q
        return pltpu.make_async_remote_copy(
            src_ref=send1.at[e, to, h, at],
            dst_ref=recv1.at[e, me_d, h, at],
            send_sem=sent.at[0],
            recv_sem=r1.at[key],
            device_id={"deep": to},
        )

    def send_modes(h_done):
        for q, chunk in enumerate(chunks):
            if (q < 2) == (h_done == 0):
                for r in (*range(2, deep), 1):
                    copy1(q, r).start()

    for h in range(halves):
        for c in range(0, nz_part, TILE):
            if (h, c) == (0, 0):
                small[0].wait()
            x_product(h, c)
        if h == 0:
            pl.semaphore_wait(barrier, deep + north - 2)
            send_modes(0)
    send_modes(1)

    for copy in small[1:]:
        copy.wait()

    coarse = waves.shape[0] // 2 - FINE

    def table_tile(c):
        cols = slice(c, c + TILE)
        cos_b = waves[2 * coarse + FINE :, cols]
        sin_b = waves[2 * coarse : 2 * coarse + FINE, cols]

        def table_step(g):
            for k in range(4):
                a = g * 4 + k
                table = waves[pl.ds(a, 1), cols] * cos_b + waves[pl.ds(coarse + a, 1), cols] * sin_b
                high, low = split(table)
                at = pl.multiple_of(a * FINE, FINE)
                t_high[pl.ds(at, FINE), cols] = high
                t_low[pl.ds(at, FINE), cols] = low

        loop(coarse // 4, table_step)

    tiles = range(0, kept_z, TILE)

    def z_tile(lhs, count, pair, c):
        at = pl.ds(pl.multiple_of(pair * 2 * nz_part, 2 * nz_part), 2 * nz_part)
        both = dot(lhs[: 2 * count], t_high[at, c : c + TILE])
        return both[:count] + both[count:] + dot(lhs[:count], t_low[at, c : c + TILE])

    def near_left(f, e):
        at = pl.ds(bases[f], half)
        block = recv1.at[e, lax.bitwise_xor(me_d, 1), :, at]
        pltpu.make_async_copy(block, block, r1.at[len(chunks) + f * each + e]).wait()
        count = halves * half * SUB
        for owner, block in ((me_d, send1), (lax.bitwise_xor(me_d, 1), recv1)):
            high, low = split(block[e, owner, :, at].reshape(count, nz_part))
            cols = pl.ds(pl.multiple_of(lax.rem(owner, 2) * nz_part, nz_part), nz_part)
            left_all[:count, cols] = high
            left_all[count:, cols] = low

    def near_tile(f, e, c):
        value = z_tile(left_all, halves * half * SUB, my_pair, c).reshape(halves, half, SUB, TILE)
        for h in range(halves):
            send2[e, pl.ds(bases[f], half), h * SUB : (h + 1) * SUB, c : c + TILE] = value[h]

    def far_left(q, pair):
        f, e, h, hs, i, count = chunks[q]
        at, rows, h = pl.ds(start_of(q), count), hs * count * SUB, pl.ds(h, hs)
        block = recv1.at[e, pl.ds(pair * 2, 2), h, at]
        pltpu.make_async_copy(block, block, r1.at[q]).wait()
        for k in range(2):
            high, low = split(recv1[e, pair * 2 + k, h, at].reshape(rows, nz_part))
            left[:rows, k * nz_part : (k + 1) * nz_part] = high
            left[rows : 2 * rows, k * nz_part : (k + 1) * nz_part] = low

    def far_tile(q, pair, c):
        f, e, h, hs, i, count = chunks[q]
        value = z_tile(left, hs * count * SUB, pair, c).reshape(hs, count, SUB, TILE)
        for k in range(hs):
            rows = slice((h + k) * SUB, (h + k + 1) * SUB)
            send2[e, pl.ds(start_of(q), count), rows, c : c + TILE] += value[k]

    def inverse_roots():
        row = lax.broadcasted_iota(jnp.int32, (share_y, TILE), 0)
        part_y = jnp.zeros((share_y, TILE), F32)
        for j in range(share_y):
            part_y = jnp.where(row == j, symbol_y[me_d * share_y + j], part_y)
        for d in range(deep):
            for e in range(each):
                part_x = symbol_x[me_n * deep * each + d * each + e]
                for c in range(0, kept_z, TILE):
                    out[d, e, :, c : c + TILE] = lax.rsqrt(part_x + part_y + symbol_z[:, c : c + TILE])

    def copy2(e, rows, cols, n):
        return pltpu.make_async_remote_copy(
            src_ref=send2.at[e, n, rows, cols],
            dst_ref=recv2.at[e, me_n, rows, cols],
            send_sem=sent.at[1],
            recv_sem=r2.at[e + (cols.start // TILE if e == last else 0)],
            device_id={"north": n},
        )

    def every(count, body):
        if count <= 8:
            for i in range(count):
                body(i)
        else:
            loop(count, body)

    def send_north(f, e, rows, cols, n):
        if f == 0:
            copy2(e, rows, cols, n).start()
        else:
            pl.when(n != me_n)(lambda: copy2(e, rows, cols, n).start())

    def send_slice(f, rows, u, n):
        send_north(f, last, rows, slice(u * TILE, (u + 1) * TILE), bases[f] + n)

    def copy3(e, p, r):
        to = lax.bitwise_xor(me_d, r)
        cols = slice(p * TILE, (p + 1) * TILE) if e == last else slice(None)
        return pltpu.make_async_remote_copy(
            src_ref=send3.at[e, to, :, cols],
            dst_ref=recv3.at[me_d, e, :, cols],
            send_sem=sent.at[2],
            recv_sem=r3.at[e + p],
            device_id={"deep": to},
        )

    def y_stage(e, p):
        cols = slice(p * TILE, (p + 1) * TILE) if e == last else slice(None)
        block = recv2.at[e, pl.ds(0, north - 1), :, cols]
        pltpu.make_async_copy(block, block, r2.at[e + p]).wait()
        for c in range(0, kept_z, TILE) if e < last else (p * TILE,):
            values = recv2[e, :, :, c : c + TILE].reshape(ny_part * north, TILE)
            both = dot(ty[...], jnp.concatenate(split(values), axis=0))
            modes = both[:kept_y] + both[kept_y:]
            send3[e, :, :, c : c + TILE] = modes.reshape(deep, share_y, TILE)
        for r in (*range(2, deep), 1):
            copy3(e, p, r).start()

    remote = jnp.where(me_n < half, half // 2, 0)
    far_chunks = sum(chunk[0] == 0 for chunk in chunks)
    rivals = [lax.rem(my_pair + k, pairs) for k in range(1, pairs)]
    whole = slice(0, kept_z)
    for q, (f, e, h, hs, i, count) in enumerate(chunks):
        lines = slice(h * SUB, (h + hs) * SUB)
        if q == 0:
            for c0 in range(0, kept_z, WIDE):
                wide = range(c0, c0 + WIDE, TILE)
                for c in wide:
                    table_tile(c)
                if c0 == 0:
                    near_left(f, e)
                for c in wide:
                    near_tile(f, e, c)
                if len(rivals) == 1:
                    if c0 == 0:
                        far_left(q, rivals[0])
                    for c in wide:
                        far_tile(q, rivals[0], c)
                    if e < last:
                        every(count, lambda k: send_north(f, e, lines, slice(c0, c0 + WIDE), bases[f] + i + k))
            inverse_roots()
            if len(rivals) == 1:
                continue
        elif h == 0 and i == 0:
            near_left(f, e)
            for c in tiles:
                near_tile(f, e, c)
        for pair in rivals:
            far_left(q, pair)
            for c in tiles:
                far_tile(q, pair, c)
        if e < last:
            every(count, lambda k: send_north(f, e, lines, whole, start_of(q) + k))
        elif f:
            for u in range(parts):
                every(count, lambda n: send_slice(f, lines, u, i + n))
        u = q - far_chunks + 1
        for v in {0: (0, 1)}.get(u, (u + 1,)) if 0 <= u < parts - 1 else ():
            every(half // 2, lambda n: send_slice(0, slice(0, ny_part), v, remote + n))
        if 0 <= u < parts:
            every(half // 2, lambda n: send_slice(0, slice(0, ny_part), u, half // 2 - remote + n))
        if f and i + count == half:
            recv2[e, me_n] = send2[e, me_n]
        if q >= len(chunks) - 2:
            @pl.when(lax.rem(me_n, half) // (half // 2) == q - len(chunks) + 2)
            def _():
                for k in range(last):
                    y_stage(k, 0)


    for p in range(parts):
        y_stage(last, p)

    for e in range(each):
        out[me_d, e] = out[me_d, e] * send3[e, me_d]
        for p in range(parts if e == last else 1):
            cols = slice(p * TILE, (p + 1) * TILE) if e == last else slice(None)
            block = recv3.at[pl.ds(0, deep - 1), e, :, cols]
            pltpu.make_async_copy(block, block, r3.at[e + p]).wait()
            for r in range(1, deep):
                owner = lax.bitwise_xor(me_d, r)
                out[owner, e, :, cols] = out[owner, e, :, cols] * recv3[owner, e, :, cols]
    for i, block in enumerate((
        send1.at[:, pl.ds(0, deep - 1)],
        send2.at[:, pl.ds(0, north - 1)],
        send3.at[:, pl.ds(0, deep - 1)],
    )):
        pltpu.make_async_copy(block, block, sent.at[i]).wait()


def on_device(source, symbol_x, symbol_y, symbol_z):
    north, deep = lax.axis_size("north"), lax.axis_size("deep")
    nx, ny_part, nz_part = source.shape
    each, halves = nx // 2 // north // deep, ny_part // SUB
    ny, nz = ny_part * north, nz_part * deep
    kept_z, share_y = nz // 2, ny // 2 // deep
    order = np.arange(nx // 2).reshape(north, deep, each).transpose(2, 1, 0).reshape(-1)
    x_high, x_low = left_table(nx)
    rows = max(ROWS, north)
    tx = jnp.asarray(np.stack([stacked(x_high[o], x_low[o]) for o in order.reshape(-1, rows)]))
    ty = jnp.asarray(stacked(*left_table(ny)))
    waves = long_tables(nz)
    remote = pl.BlockSpec(memory_space=pltpu.HBM)
    rows = SUB * north
    chunks = each * halves + 1 + 2 * each
    operands = (source, tx, ty, waves, symbol_x, symbol_y, symbol_z[None, :])
    buffers = [
        *((t.shape, t.dtype) for t in (tx, ty, waves)),
        ((1, nz), F32),
        ((halves, nx, SUB, nz_part), F32),
        ((SUB, 2 * nx, TILE), BF16),
        ((each, deep, halves, north, SUB, nz_part), F32),
        ((each, deep, halves, north, SUB, nz_part), F32),
        ((each, north, ny_part, kept_z), F32),
        ((each, north, ny_part, kept_z), F32),
        ((each, deep, share_y, kept_z), F32),
        ((deep, each, share_y, kept_z), F32),
        ((nz, kept_z), BF16),
        ((nz, kept_z), BF16),
        ((halves * rows, 2 * nz_part), BF16),
        ((rows, 2 * nz_part), BF16),
    ]
    used = sum(int(np.prod(shape)) * jnp.dtype(kind).itemsize for shape, kind in buffers)
    limit = MOST - SPARE if used < MOST - 2 * SPARE else MOST
    v = pl.pallas_call(
        functools.partial(kernel, north, deep, each),
        out_shape=jax.ShapeDtypeStruct((deep, each, share_y, kept_z), F32),
        in_specs=[remote] * len(operands),
        out_specs=pl.BlockSpec(memory_space=pltpu.VMEM),
        scratch_shapes=[pltpu.VMEM(shape, kind) for shape, kind in buffers]
        + [
            pltpu.SMEM(symbol_x.shape, F32),
            pltpu.SMEM(symbol_y.shape, F32),
            pltpu.SemaphoreType.DMA((halves * nz_part // TILE,)),
            pltpu.SemaphoreType.DMA((len(operands) - 1,)),
        ]
        + [
            pltpu.SemaphoreType.DMA((count,))
            for count in (3, chunks + 2 * each, each + kept_z // TILE, each + kept_z // TILE)
        ],
        compiler_params=pltpu.CompilerParams(
            collective_id=0, has_side_effects=True, vmem_limit_bytes=limit
        ),
    )(*(pltpu.with_memory_space_constraint(operand, pltpu.HBM) for operand in operands))
    return v.reshape(deep * each, share_y, kept_z)


def solution(mesh):
    in_specs = (P(None, "north", "deep"), P(), P(), P())
    out_specs = P("north", "deep", None)
    return jax.shard_map(
        on_device, mesh=mesh, in_specs=in_specs, out_specs=out_specs, check_vma=False
    )
```

```python
import functools

import jax
import jax.numpy as jnp
import numpy as np
from jax import lax
from jax.experimental import pallas as pl
from jax.experimental.pallas import tpu as pltpu
from jax.sharding import PartitionSpec as P

F32, BF16 = jnp.float32, jnp.bfloat16
FINE = 32
TILE = 256
WIDE = 512
SUB = 8
ROWS = 64
MOST = 67043328
SPARE = 14 << 20


def angles(rows, modes, count):
    rank = np.outer(rows, modes) % (2 * count + 2)
    return np.pi / (count + 1) * rank


def split_np(table):
    high = table.astype(np.float32).astype(BF16)
    low = (table - high.astype(np.float64)).astype(np.float32).astype(BF16)
    return high, low


def left_table(count):
    gain = (2.0 / (count + 1)) ** 0.5
    table = np.sin(angles(np.arange(1, count // 2 + 1), np.arange(1, count + 1), count)) * gain
    return split_np(table)


def stacked(high, low):
    return np.block([[high, high], [low, np.zeros_like(low)]])


def long_tables(count):
    modes = np.arange(1, count // 2 + 1)
    gain = (2.0 / (count + 1)) ** 0.5
    coarse = angles(np.arange(0, count, FINE), modes, count)
    step = angles(np.arange(1, FINE + 1), modes, count)
    parts = (np.sin(coarse) * gain, np.cos(coarse) * gain, np.sin(step), np.cos(step))
    return jnp.asarray(np.concatenate(parts).astype(np.float32))


def split(values):
    high = values.astype(BF16)
    return high, (values - high.astype(F32)).astype(BF16)


def dot(a, b):
    return jnp.dot(a, b, preferred_element_type=F32)


def loop(count, body):
    if count == 1:
        body(0)
    else:
        lax.fori_loop(0, count, lambda i, c: (body(i), c)[1], 0)


def kernel(
    north, deep, each,
    src, tx_in, ty_in, *rest,
):
    waves_in, sx_in, sy_in, sz_in, out = rest[:5]
    tx, ty, waves, symbol_z = rest[5:9]
    field, turned, send1, recv1, send2, recv2, send3, recv3, t_high, t_low, left_all, left = rest[9:21]
    symbol_x, symbol_y, fs, ins, sent, r1, r2, r3 = rest[21:]

    me_n, me_d = lax.axis_index("north"), lax.axis_index("deep")
    nx, ny_part, nz_part = src.shape
    halves = ny_part // SUB
    kept_z = t_high.shape[1]
    kept_y = ny_part * north // 2
    share_y = kept_y // deep
    half = north // 2
    pairs = deep // 2
    my_pair = me_d // 2
    far = jnp.where(me_n < half, half, 0)
    bases = (far, half - far)
    last = each - 1
    parts = kept_z // TILE

    loads = {}
    small = []

    def fetch(what, to):
        copy = pltpu.make_async_copy(what, to, ins.at[len(small)])
        copy.start()
        small.append(copy)

    fetch(tx_in, tx)
    for i, (h, c) in enumerate((h, c) for h in range(halves) for c in range(0, nz_part, TILE)):
        loads[h, c] = pltpu.make_async_copy(
            src.at[:, h * SUB : (h + 1) * SUB, c : c + TILE], field.at[h, :, :, c : c + TILE], fs.at[i]
        )
        loads[h, c].start()
    for what, to in zip(
        (waves_in, ty_in, sx_in, sy_in, sz_in),
        (waves, ty, symbol_x, symbol_y, symbol_z),
    ):
        fetch(what, to)

    barrier = pltpu.get_barrier_semaphore()
    for r in range(1, deep):
        pl.semaphore_signal(barrier, inc=1, device_id={"deep": lax.rem(me_d + r, deep)})
    for r in range(1, north):
        pl.semaphore_signal(barrier, inc=1, device_id={"north": lax.rem(me_n + r, north)})

    def x_product(h, c):
        loads[h, c].wait()
        block = min(nx, 128)

        def turn(g):
            for k in range(0, block, 16):
                at = pl.multiple_of(g * block + k, 16)
                high, low = split(jnp.swapaxes(field[h, pl.ds(at, 16), :, c : c + TILE], 0, 1))
                turned[:, pl.ds(at, 16), :] = high
                turned[:, pl.ds(pl.multiple_of(nx + at, 16), 16), :] = low

        loop(nx // block, turn)
        rows = tx.shape[1] // 2
        group = rows // north

        def modes_of(g):
            modes = []
            for y in range(SUB):
                both = dot(tx[g], turned[y])
                modes.append(both[:rows] + both[rows:])
            for k in range(group):
                block = jnp.stack([m[k * north : (k + 1) * north] for m in modes])
                ed = g * group + k
                send1[ed // deep, lax.rem(ed, deep), h, :, :, c : c + TILE] = jnp.swapaxes(block, 0, 1)

        loop(tx.shape[0], modes_of)

    chunks = []
    for e in range(each):
        for h in range(halves):
            cut = half if chunks else half // 2
            chunks += [(0, e, h, 1, i, cut) for i in range(0, half, cut)]
    for e in range(each):
        cut = half // 2 if e < last else 1
        chunks += [(1, e, 0, halves, i, cut) for i in range(0, half, cut)]

    first_pair = lax.rem(me_n, half) < half // 2

    def start_of(q):
        f, e, _, _, i, count = chunks[q]
        if f and e < last:
            i = jnp.where(me_n < half, i, half - count - i)
        elif f:
            rank = lax.rem(me_n, half)
            turns = [lax.bitwise_xor(rank, k) for k in range(half)]
            if half == 4:
                i = jnp.where(first_pair, (turns[1], 2, 3, rank)[i], (0, 1, turns[1], rank)[i])
            else:
                i = turns[(i + 1) % half]
        return bases[f] + i

    def copy1(q, r):
        f, e, h, hs, i, count = chunks[q]
        at, h = pl.ds(start_of(q), count), pl.ds(h, hs)
        to = lax.bitwise_xor(me_d, r)
        key = len(chunks) + f * each + e if r == 1 else q
        return pltpu.make_async_remote_copy(
            src_ref=send1.at[e, to, h, at],
            dst_ref=recv1.at[e, me_d, h, at],
            send_sem=sent.at[0],
            recv_sem=r1.at[key],
            device_id={"deep": to},
        )

    def send_modes(h_done):
        for q, chunk in enumerate(chunks):
            if (q < 2) == (h_done == 0):
                for r in (*range(2, deep), 1):
                    copy1(q, r).start()

    for h in range(halves):
        for c in range(0, nz_part, TILE):
            if (h, c) == (0, 0):
                small[0].wait()
            x_product(h, c)
        if h == 0:
            pl.semaphore_wait(barrier, deep + north - 2)
            send_modes(0)
    send_modes(1)

    for copy in small[1:]:
        copy.wait()

    coarse = waves.shape[0] // 2 - FINE

    def table_tile(c):
        cols = slice(c, c + TILE)
        cos_b = waves[2 * coarse + FINE :, cols]
        sin_b = waves[2 * coarse : 2 * coarse + FINE, cols]

        def table_step(g):
            for k in range(4):
                a = g * 4 + k
                table = waves[pl.ds(a, 1), cols] * cos_b + waves[pl.ds(coarse + a, 1), cols] * sin_b
                high, low = split(table)
                at = pl.multiple_of(a * FINE, FINE)
                t_high[pl.ds(at, FINE), cols] = high
                t_low[pl.ds(at, FINE), cols] = low

        loop(coarse // 4, table_step)

    tiles = range(0, kept_z, TILE)

    def z_tile(lhs, count, pair, c):
        at = pl.ds(pl.multiple_of(pair * 2 * nz_part, 2 * nz_part), 2 * nz_part)
        both = dot(lhs[: 2 * count], t_high[at, c : c + TILE])
        return both[:count] + both[count:] + dot(lhs[:count], t_low[at, c : c + TILE])

    def near_left(f, e):
        at = pl.ds(bases[f], half)
        block = recv1.at[e, lax.bitwise_xor(me_d, 1), :, at]
        pltpu.make_async_copy(block, block, r1.at[len(chunks) + f * each + e]).wait()
        count = halves * half * SUB
        for owner, block in ((me_d, send1), (lax.bitwise_xor(me_d, 1), recv1)):
            high, low = split(block[e, owner, :, at].reshape(count, nz_part))
            cols = pl.ds(pl.multiple_of(lax.rem(owner, 2) * nz_part, nz_part), nz_part)
            left_all[:count, cols] = high
            left_all[count:, cols] = low

    def near_tile(f, e, c):
        value = z_tile(left_all, halves * half * SUB, my_pair, c).reshape(halves, half, SUB, TILE)
        for h in range(halves):
            send2[e, pl.ds(bases[f], half), h * SUB : (h + 1) * SUB, c : c + TILE] = value[h]

    def far_left(q, pair):
        f, e, h, hs, i, count = chunks[q]
        at, rows, h = pl.ds(start_of(q), count), hs * count * SUB, pl.ds(h, hs)
        block = recv1.at[e, pl.ds(pair * 2, 2), h, at]
        pltpu.make_async_copy(block, block, r1.at[q]).wait()
        for k in range(2):
            high, low = split(recv1[e, pair * 2 + k, h, at].reshape(rows, nz_part))
            left[:rows, k * nz_part : (k + 1) * nz_part] = high
            left[rows : 2 * rows, k * nz_part : (k + 1) * nz_part] = low

    def far_tile(q, pair, c):
        f, e, h, hs, i, count = chunks[q]
        value = z_tile(left, hs * count * SUB, pair, c).reshape(hs, count, SUB, TILE)
        for k in range(hs):
            rows = slice((h + k) * SUB, (h + k + 1) * SUB)
            send2[e, pl.ds(start_of(q), count), rows, c : c + TILE] += value[k]

    def inverse_roots():
        row = lax.broadcasted_iota(jnp.int32, (share_y, TILE), 0)
        part_y = jnp.zeros((share_y, TILE), F32)
        for j in range(share_y):
            part_y = jnp.where(row == j, symbol_y[me_d * share_y + j], part_y)
        for d in range(deep):
            for e in range(each):
                part_x = symbol_x[me_n * deep * each + d * each + e]
                for c in range(0, kept_z, TILE):
                    out[d, e, :, c : c + TILE] = lax.rsqrt(part_x + part_y + symbol_z[:, c : c + TILE])

    def copy2(e, rows, cols, n):
        return pltpu.make_async_remote_copy(
            src_ref=send2.at[e, n, rows, cols],
            dst_ref=recv2.at[e, me_n, rows, cols],
            send_sem=sent.at[1],
            recv_sem=r2.at[e + (cols.start // TILE if e == last else 0)],
            device_id={"north": n},
        )

    def every(count, body):
        if count <= 8:
            for i in range(count):
                body(i)
        else:
            loop(count, body)

    def send_north(f, e, rows, cols, n):
        if f == 0:
            copy2(e, rows, cols, n).start()
        else:
            pl.when(n != me_n)(lambda: copy2(e, rows, cols, n).start())

    def send_slice(f, rows, u, n):
        send_north(f, last, rows, slice(u * TILE, (u + 1) * TILE), bases[f] + n)

    def copy3(e, p, r):
        to = lax.bitwise_xor(me_d, r)
        cols = slice(p * TILE, (p + 1) * TILE) if e == last else slice(None)
        return pltpu.make_async_remote_copy(
            src_ref=send3.at[e, to, :, cols],
            dst_ref=recv3.at[me_d, e, :, cols],
            send_sem=sent.at[2],
            recv_sem=r3.at[e + p],
            device_id={"deep": to},
        )

    def y_stage(e, p):
        cols = slice(p * TILE, (p + 1) * TILE) if e == last else slice(None)
        block = recv2.at[e, pl.ds(0, north - 1), :, cols]
        pltpu.make_async_copy(block, block, r2.at[e + p]).wait()
        for c in range(0, kept_z, TILE) if e < last else (p * TILE,):
            values = recv2[e, :, :, c : c + TILE].reshape(ny_part * north, TILE)
            both = dot(ty[...], jnp.concatenate(split(values), axis=0))
            modes = both[:kept_y] + both[kept_y:]
            send3[e, :, :, c : c + TILE] = modes.reshape(deep, share_y, TILE)
        for r in (*range(2, deep), 1):
            copy3(e, p, r).start()

    remote = jnp.where(me_n < half, half // 2, 0)
    far_chunks = sum(chunk[0] == 0 for chunk in chunks)
    rivals = [lax.rem(my_pair + k, pairs) for k in range(1, pairs)]
    whole = slice(0, kept_z)
    for q, (f, e, h, hs, i, count) in enumerate(chunks):
        lines = slice(h * SUB, (h + hs) * SUB)
        if q == 0:
            for c0 in range(0, kept_z, WIDE):
                wide = range(c0, c0 + WIDE, TILE)
                for c in wide:
                    table_tile(c)
                if c0 == 0:
                    near_left(f, e)
                for c in wide:
                    near_tile(f, e, c)
                if len(rivals) == 1:
                    if c0 == 0:
                        far_left(q, rivals[0])
                    for c in wide:
                        far_tile(q, rivals[0], c)
                    if e < last:
                        every(count, lambda k: send_north(f, e, lines, slice(c0, c0 + WIDE), bases[f] + i + k))
            inverse_roots()
            if len(rivals) == 1:
                continue
        elif h == 0 and i == 0:
            near_left(f, e)
            for c in tiles:
                near_tile(f, e, c)
        for pair in rivals:
            far_left(q, pair)
            for c in tiles:
                far_tile(q, pair, c)
        if e < last:
            every(count, lambda k: send_north(f, e, lines, whole, start_of(q) + k))
        elif f and i + 1 < half:
            for u in range(parts):
                copy2(e, lines, slice(u * TILE, (u + 1) * TILE), start_of(q)).start()
        u = q - far_chunks + 1
        for v in {0: (0, 1)}.get(u, (u + 1,)) if 0 <= u < parts - 1 else ():
            every(half // 2, lambda n: send_slice(0, slice(0, ny_part), v, remote + n))
        if 0 <= u < parts:
            every(half // 2, lambda n: send_slice(0, slice(0, ny_part), u, half // 2 - remote + n))
        if f and i + count == half:
            recv2[e, me_n] = send2[e, me_n]
        if q in (len(chunks) - 3, len(chunks) - 1):
            @pl.when(first_pair if q < len(chunks) - 1 else jnp.logical_not(first_pair))
            def _():
                for k in range(last):
                    y_stage(k, 0)


    for p in range(parts):
        y_stage(last, p)

    for e in range(each):
        out[me_d, e] = out[me_d, e] * send3[e, me_d]
        for p in range(parts if e == last else 1):
            cols = slice(p * TILE, (p + 1) * TILE) if e == last else slice(None)
            block = recv3.at[pl.ds(0, deep - 1), e, :, cols]
            pltpu.make_async_copy(block, block, r3.at[e + p]).wait()
            for r in range(1, deep):
                owner = lax.bitwise_xor(me_d, r)
                out[owner, e, :, cols] = out[owner, e, :, cols] * recv3[owner, e, :, cols]
    for i, block in enumerate((
        send1.at[:, pl.ds(0, deep - 1)],
        send2.at[:, pl.ds(0, north - 1)],
        send3.at[:, pl.ds(0, deep - 1)],
    )):
        pltpu.make_async_copy(block, block, sent.at[i]).wait()


def on_device(source, symbol_x, symbol_y, symbol_z):
    north, deep = lax.axis_size("north"), lax.axis_size("deep")
    nx, ny_part, nz_part = source.shape
    each, halves = nx // 2 // north // deep, ny_part // SUB
    ny, nz = ny_part * north, nz_part * deep
    kept_z, share_y = nz // 2, ny // 2 // deep
    order = np.arange(nx // 2).reshape(north, deep, each).transpose(2, 1, 0).reshape(-1)
    x_high, x_low = left_table(nx)
    rows = max(ROWS, north)
    tx = jnp.asarray(np.stack([stacked(x_high[o], x_low[o]) for o in order.reshape(-1, rows)]))
    ty = jnp.asarray(stacked(*left_table(ny)))
    waves = long_tables(nz)
    remote = pl.BlockSpec(memory_space=pltpu.HBM)
    rows = SUB * north
    chunks = each * halves + 1 + 2 * (each - 1) + north // 2
    operands = (source, tx, ty, waves, symbol_x, symbol_y, symbol_z[None, :])
    buffers = [
        *((t.shape, t.dtype) for t in (tx, ty, waves)),
        ((1, nz), F32),
        ((halves, nx, SUB, nz_part), F32),
        ((SUB, 2 * nx, TILE), BF16),
        ((each, deep, halves, north, SUB, nz_part), F32),
        ((each, deep, halves, north, SUB, nz_part), F32),
        ((each, north, ny_part, kept_z), F32),
        ((each, north, ny_part, kept_z), F32),
        ((each, deep, share_y, kept_z), F32),
        ((deep, each, share_y, kept_z), F32),
        ((nz, kept_z), BF16),
        ((nz, kept_z), BF16),
        ((halves * rows, 2 * nz_part), BF16),
        ((rows, 2 * nz_part), BF16),
    ]
    used = sum(int(np.prod(shape)) * jnp.dtype(kind).itemsize for shape, kind in buffers)
    limit = MOST - SPARE if used < MOST - 2 * SPARE else MOST
    v = pl.pallas_call(
        functools.partial(kernel, north, deep, each),
        out_shape=jax.ShapeDtypeStruct((deep, each, share_y, kept_z), F32),
        in_specs=[remote] * len(operands),
        out_specs=pl.BlockSpec(memory_space=pltpu.VMEM),
        scratch_shapes=[pltpu.VMEM(shape, kind) for shape, kind in buffers]
        + [
            pltpu.SMEM(symbol_x.shape, F32),
            pltpu.SMEM(symbol_y.shape, F32),
            pltpu.SemaphoreType.DMA((halves * nz_part // TILE,)),
            pltpu.SemaphoreType.DMA((len(operands) - 1,)),
        ]
        + [
            pltpu.SemaphoreType.DMA((count,))
            for count in (3, chunks + 2 * each, each + kept_z // TILE, each + kept_z // TILE)
        ],
        compiler_params=pltpu.CompilerParams(
            collective_id=0, has_side_effects=True, vmem_limit_bytes=limit
        ),
    )(*(pltpu.with_memory_space_constraint(operand, pltpu.HBM) for operand in operands))
    return v.reshape(deep * each, share_y, kept_z)


def solution(mesh):
    in_specs = (P(None, "north", "deep"), P(), P(), P())
    out_specs = P("north", "deep", None)
    return jax.shard_map(
        on_device, mesh=mesh, in_specs=in_specs, out_specs=out_specs, check_vma=False
    )
```
